256 devices in a mesh: ctx: 32 (over z_lo, x, y), fsdp: 8 (over z_hi, core).
Axes of the slice: x: 4, y: 4, z: 8 (z_hi: 4, z_lo: 2; z = z_hi * 2 + z_lo), core: 2. Of those that a mesh axis runs over, the one named last changes fastest.
Arguments:
- tokens: bfloat16 [8, 4096, 4096], P('fsdp', 'ctx'), may hold values from -6 to 6
- positions: int32 [8, 4096], P('fsdp', 'ctx'), may hold values from 0 to 4095, as said below
- norm_gain: float32 [4096], replicated, may hold values from 0.5 to 1.5
- query_weight: bfloat16 [4096, 2048], P('fsdp'), may hold values from -1 to 1
- key_weight: bfloat16 [4096, 512], P('fsdp'), may hold values from -1 to 1
- value_matrix: bfloat16 [4096, 512], P('fsdp'), may hold values from -0.09375 to 0.09375
Outputs:
- attended: bfloat16 [8, 4096, 2048], P('fsdp', 'ctx')
The draws below stay inside these ranges and needn't reach their ends.
Inputs may be any that keep to these rules, and one draw needn't show every extreme that they name: In each sequence every position from 0 to 4095 appears once, in runs of 64 consecutive rising positions that begin at multiples of 64 in the array.
All inputs are finite; a program needn't handle non-finite values.
Results may differ from the reference program's by a relative error of at most 0.012.
The reference program's roundings to bfloat16 on the way count: a program that leaves them out, or rounds other values in their place, can miss the bound.
Values may be sent and summed in bfloat16 or wider, within the bound.
A program may use at most 128 MiB of HBM per device.

```python
import jax
import jax.numpy as jnp
from jax import lax

MODEL_WIDTH = 4096
QUERY_HEADS = 16
KEY_VALUE_HEADS = 4
HEAD_SIZE = 128
TOK_DEV = 128
SEQUENCE_COUNT = 8
SEQUENCE_LENGTH = 4096


def shared_weights(key):
    common = jax.random.truncated_normal(jax.random.fold_in(key, 11), -6.0, 6.0, (MODEL_WIDTH, QUERY_HEADS * HEAD_SIZE), jnp.float32) / jnp.sqrt(1.0 * MODEL_WIDTH)
    separate_streams = jax.random.truncated_normal(jax.random.fold_in(key, 12), -6.0, 6.0, (MODEL_WIDTH, KEY_VALUE_HEADS * HEAD_SIZE), jnp.float32) / jnp.sqrt(1.0 * MODEL_WIDTH)
    query_vectors = common
    key_part = separate_streams
    return (jnp.clip(query_vectors, -1.0, 1.0), jnp.clip(key_part, -1.0, 1.0))


def draw_query_weight(key, part):
    return shared_weights(key)[0].astype(jnp.bfloat16)


def draw_key_weight(key, part):
    return shared_weights(key)[1].astype(jnp.bfloat16)


def draw_positions(key, part):
    block_size = TOK_DEV // 2
    block_count = SEQUENCE_LENGTH // block_size
    orders = jax.vmap(lambda sequence: jax.random.permutation(jax.random.fold_in(key, sequence), block_count))(jnp.arange(SEQUENCE_COUNT, dtype=jnp.int32))
    places = orders[:, :, None] * block_size + jnp.arange(block_size, dtype=jnp.int32)[None, None, :]
    return places.reshape(SEQUENCE_COUNT, SEQUENCE_LENGTH).astype(jnp.int32)


def shard_levels(rng, extent, pieces, low, largest):
    level, own = 1.0, jax.random.fold_in(rng, 6)
    for axis_at, blocks in pieces:
        heights = jnp.exp(jax.random.uniform(jax.random.fold_in(own, axis_at), (blocks,), jnp.float32, low / len(pieces), largest / len(pieces)))
        level = level * jnp.repeat(heights, extent[axis_at] // blocks).reshape([-1 if axis == axis_at else 1 for axis in range(len(extent))])
    return level


def gaussian(own_key, dims, scale, most, pieces=(), kind=jnp.bfloat16):
    result = jax.random.normal(own_key, dims, jnp.float32) * scale
    if len(pieces) > 0:
        result = shard_levels(own_key, dims, pieces, -0.22, 0.18) * result
    return jnp.clip(result, min=-most, max=most).astype(kind)


def setup_inputs(seed: int = 0) -> dict:
    key_list = jax.random.split(jax.random.key(seed), 7)
    tokens = gaussian(key_list[0], (SEQUENCE_COUNT, SEQUENCE_LENGTH, MODEL_WIDTH), 1.0, 6.0, ((0, 8), (1, 32)))
    positions = draw_positions(jax.random.fold_in(key_list[6], 71), 0)
    norm_gain = jnp.clip(1.0 + 0.1 * jax.random.normal(key_list[2], (MODEL_WIDTH,), jnp.float32), 0.5, 1.5)
    query_weight = draw_query_weight(jax.random.fold_in(key_list[6], 71), 0)
    key_weight = draw_key_weight(jax.random.fold_in(key_list[6], 71), 0)
    value_matrix = gaussian(key_list[5], (MODEL_WIDTH, KEY_VALUE_HEADS * HEAD_SIZE), MODEL_WIDTH ** -0.5, 0.09375, ((0, 8),))
    return dict(tokens=tokens, positions=positions, norm_gain=norm_gain, query_weight=query_weight, key_weight=key_weight, value_matrix=value_matrix)


EPS = 1e-05
BASE = 500000.0
MASK_FLOOR = -1e+30

def normalize(tokens, norm_gain):
    values = tokens.astype(jnp.float32)
    inverse = lax.rsqrt(lax.optimization_barrier(jnp.mean(values * values, axis=-1, keepdims=True)) + EPS)
    return (values * inverse * norm_gain.astype(jnp.float32)).astype(jnp.bfloat16)

def rope_tables(places, head_dim):
    half_dim = head_dim // 2
    frequency = BASE ** (-(jnp.arange(half_dim, dtype=jnp.float32) * 2.0) / head_dim)
    angles = places.astype(jnp.float32)[:, None] * frequency[None, :]
    return (jnp.cos(angles), jnp.sin(angles))

def apply_rotation(x, cosine_table_rows, sine_table_rows):
    half_dim = x.shape[-1] // 2
    first_half = x[..., :half_dim]
    second_half = x[..., half_dim:]
    cosine_part = cosine_table_rows[:, None, :]
    sine_part = sine_table_rows[:, None, :]
    return jnp.concatenate([first_half * cosine_part - second_half * sine_part, second_half * cosine_part + first_half * sine_part], axis=-1)

def reference(tokens, positions, norm_gain, query_weight, key_weight, value_matrix):
    query_groups = QUERY_HEADS // KEY_VALUE_HEADS
    normed = normalize(tokens, norm_gain).reshape(SEQUENCE_COUNT * SEQUENCE_LENGTH, MODEL_WIDTH)
    query_unrotated = jnp.dot(normed, query_weight, preferred_element_type=jnp.float32)
    key_unrotated = jnp.dot(normed, key_weight, preferred_element_type=jnp.float32)
    value_projected = jnp.dot(normed, value_matrix, preferred_element_type=jnp.float32)
    cosine_table_rows, sine_table_rows = rope_tables(positions.reshape(SEQUENCE_COUNT * SEQUENCE_LENGTH), HEAD_SIZE)
    query_complete = apply_rotation(query_unrotated.reshape(SEQUENCE_COUNT * SEQUENCE_LENGTH, QUERY_HEADS, HEAD_SIZE), cosine_table_rows, sine_table_rows).astype(jnp.bfloat16).reshape(SEQUENCE_COUNT, SEQUENCE_LENGTH, KEY_VALUE_HEADS, query_groups, HEAD_SIZE)
    key_complete = apply_rotation(key_unrotated.reshape(SEQUENCE_COUNT * SEQUENCE_LENGTH, KEY_VALUE_HEADS, HEAD_SIZE), cosine_table_rows, sine_table_rows).astype(jnp.bfloat16).reshape(SEQUENCE_COUNT, SEQUENCE_LENGTH, KEY_VALUE_HEADS, HEAD_SIZE)
    value_complete = value_projected.astype(jnp.bfloat16).reshape(SEQUENCE_COUNT, SEQUENCE_LENGTH, KEY_VALUE_HEADS, HEAD_SIZE)
    block_size = min(512, SEQUENCE_LENGTH)
    block_count = SEQUENCE_LENGTH // block_size

    def one_sequence(inputs):
        query_seq, key_seq, value_seq, seq_places = inputs
        key_float = key_seq.astype(jnp.float32)
        value_float = value_seq.astype(jnp.float32)

        def one_block(block_index):
            begin = (block_index * block_size).astype(jnp.int32)
            query_block = lax.dynamic_slice_in_dim(query_seq, begin, block_size, 0).astype(jnp.float32)
            query_places = lax.dynamic_slice_in_dim(seq_places, begin, block_size, 0)
            scores = jnp.einsum('qhgd,khd->qhgk', query_block, key_float, precision=lax.Precision.HIGHEST) * HEAD_SIZE ** (-0.5)
            allowed = (seq_places[None, :] <= query_places[:, None])[:, None, None, :]
            scores = jnp.where(allowed, scores, MASK_FLOOR)
            maximum = lax.optimization_barrier(jnp.max(scores, axis=-1, keepdims=True))
            weights = jnp.where(allowed, jnp.exp(scores - maximum), 0.0)
            denominator = lax.optimization_barrier(jnp.sum(weights, axis=-1))
            rounded = weights.astype(jnp.bfloat16).astype(jnp.float32)
            mixed = jnp.einsum('qhgk,khd->qhgd', rounded, value_float, precision=lax.Precision.HIGHEST)
            return (mixed / denominator[..., None]).astype(jnp.bfloat16).reshape(block_size, QUERY_HEADS * HEAD_SIZE)
        blocks = lax.map(one_block, jnp.arange(block_count, dtype=jnp.int32))
        return blocks.reshape(SEQUENCE_LENGTH, QUERY_HEADS * HEAD_SIZE)
    return lax.map(one_sequence, (query_complete, key_complete, value_complete, positions))
```

```python
import math

import jax
import jax.numpy as jnp
from jax import lax
from jax.experimental import pallas as pl
from jax.experimental.pallas import tpu as pltpu
from jax.sharding import PartitionSpec as P

HEAD = 128
GROUP = 4
EPS = 1e-05
BASE = 500000.0
FLOOR = -1e30
LOG2E = math.log2(math.e)
F32, BF16 = jnp.float32, jnp.bfloat16


def rope_tables(places):
    half = HEAD // 2
    frequency = BASE ** (-(jnp.arange(half, dtype=F32) * 2.0) / HEAD)
    angles = places.astype(F32)[:, None] * frequency[None, :]
    return jnp.concatenate([jnp.cos(angles), jnp.sin(angles)], axis=1)


def around(n):
    return jnp.where(n == 0, 0, jnp.where(n == 1, 3, jnp.where(n == 2, 1, 2)))


class PlaneGather:
    def __init__(self, at, piece, send_sem, recv_sem):
        self.at, self.piece, self.ss, self.rs = at, piece, send_sem, recv_sem

    def slot(self, g, da, db):
        dx, dy = (da, db) if g == 0 else (db, da)
        return lax.rem(self.at["x"] + dx, 4) * 4 + lax.rem(self.at["y"] + dy, 4)

    def neighbour(self, g, axis, step):
        along_x = (axis == 0) == (g == 0)
        dx, dy = (step, 0) if along_x else (0, step)
        ctx = self.at["zl"] * 16 + lax.rem(self.at["x"] + dx, 4) * 4 + lax.rem(self.at["y"] + dy, 4)
        return {"ctx": ctx, "fsdp": self.at["f"]}

    def copy(self, g, n, h, p, device):
        ref = self.piece(g, h, p)
        return pltpu.make_async_remote_copy(
            src_ref=ref, dst_ref=ref, send_sem=self.ss.at[g, n], recv_sem=self.rs.at[g, p, h],
            device_id=device, device_id_type=pl.DeviceIdType.MESH)

    def send(self, g, n, h, p, axis, step):
        self.copy(g, n, h, p, self.neighbour(g, axis, step)).start()

    def arrived(self, g, h, p):
        self.copy(g, 0, h, p, self.neighbour(g, 0, 1)).wait_recv()

    def second(self, g, n, da):
        p = self.slot(g, da, 0)
        for h in (0, 1):
            self.send(g, 6 + n * 6 + 2 * h, h, p, 1, 1)
            self.send(g, 6 + n * 6 + 2 * h + 1, h, p, 1, 3)

    def s0(self, g):
        p = self.slot(g, 0, 0)
        for h in (0, 1):
            self.send(g, 2 * h, h, p, 0, 1)
            self.send(g, 2 * h + 1, h, p, 0, 3)
        self.second(g, 0, 0)

    def s1(self, g):
        for n, d, h, step in ((1, 3, 0, 1), (2, 1, 1, 3)):
            p = self.slot(g, d, 0)
            self.arrived(g, h, p)
            self.send(g, 3 + n, h, p, 0, step)
            self.arrived(g, 1 - h, p)
            self.second(g, n, d)

    def s2(self, g):
        p = self.slot(g, 2, 0)
        for h in (0, 1):
            self.arrived(g, h, p)
        self.second(g, 3, 2)

    def s3(self, g, n):
        d = around(n)
        for db, h, step in ((3, 0, 1), (1, 1, 3)):
            p = self.slot(g, d, db)
            self.arrived(g, h, p)
            self.send(g, 6 + n * 6 + 4 + h, h, p, 1, step)
        for db, h in ((3, 1), (1, 0)):
            self.arrived(g, h, self.slot(g, d, db))

    def s4(self, g, n):
        for h in (0, 1):
            self.arrived(g, h, self.slot(g, around(n), 2))

    def finish(self):
        for g in (0, 1):
            for n in range(30):
                self.copy(g, n, 0, 0, self.neighbour(g, 0, 1)).wait_send()


def rotate(u, table):
    turned = pltpu.roll(table, 64, 1)
    first = lax.broadcasted_iota(jnp.int32, table.shape, 1) < 64
    cosine = jnp.where(first, table, turned)
    sine = jnp.where(first, -turned, table)
    return u * cosine + pltpu.roll(u, 64, 1) * sine


def kernel(tok, gain, cs, qw, kw, vw, out, tq, csq, wkv, wq, kvb, qt, acc, top, proj, osend, obuf,
           loc_s, zs, zr, ws, wr, ts, tr, fs, fr, s_a, r_a, s_b, r_b, s_c, r_c, os_, or_, outs_):
    c, f = lax.axis_index("ctx"), lax.axis_index("fsdp")
    zl, x, y = c // 16, lax.rem(c // 4, 4), lax.rem(c, 4)
    zh, k = f // 2, lax.rem(f, 2)
    col = x * 4 + y
    at = {"zl": zl, "x": x, "y": y, "f": f}
    mine, head = k * 2 + zl, zl * 2 + k

    def device(zh_, zl_, k_):
        return {"ctx": zl_ * 16 + col, "fsdp": zh_ * 2 + k_}

    def remote(src, dst, ss, rs, dev):
        return pltpu.make_async_remote_copy(src_ref=src, dst_ref=dst, send_sem=ss, recv_sem=rs, device_id=dev,
                                            device_id_type=pl.DeviceIdType.MESH)

    core = device(zh, zl, 1 - k)
    chip = device(zh, 1 - zl, k)
    diagonal = device(zh, 1 - zl, 1 - k)
    step_a = 1 + 2 * zl
    slab_a = lax.rem(zh + 4 - step_a, 4)
    slab_c = lax.rem(zh + step_a, 4)
    slab_b = lax.rem(zh + 2, 4)
    push_to = [(step_a, slab_a, zl_, k_) for zl_ in (0, 1) for k_ in (0, 1)] + [(2, slab_b, 1 - zl, k_) for k_ in (0, 1)]

    barrier = pltpu.get_barrier_semaphore()
    ring = PlaneGather(at, None, None, None)
    friends = [core, chip, diagonal]
    friends += [ring.neighbour(0, axis, step) for axis in (0, 1) for step in (1, 3)]
    friends += [device(slab_a, zl_, k_) for zl_ in (0, 1) for k_ in (0, 1)]
    friends += [device(slab_b, 1 - zl, k_) for k_ in (0, 1)]
    friends += [device(slab_c, zl, k_) for k_ in (0, 1)]
    for friend in friends:
        pl.semaphore_signal(barrier, inc=1, device_id=friend, device_id_type=pl.DeviceIdType.MESH)

    own = [
        pltpu.make_async_copy(kw.at[:, pl.ds(pl.multiple_of(head * 128, 128), 128)], wkv.at[k, :, pl.ds(0, 128)], loc_s.at[0]),
        pltpu.make_async_copy(vw.at[:, pl.ds(pl.multiple_of(head * 128, 128), 128)], wkv.at[k, :, pl.ds(128, 128)], loc_s.at[1]),
        pltpu.make_async_copy(qw.at[:, pl.ds(pl.multiple_of(head * 512, 512), 512)], wq.at[k], loc_s.at[2]),
    ]
    for copy in own:
        copy.start()

    def norm_rows(i, _):
        rows = pl.ds(pl.multiple_of(i * 16, 16), 16)
        values = tok[rows, :].astype(F32)
        inverse = lax.rsqrt(jnp.mean(values * values, axis=-1, keepdims=True) + EPS)
        tq[mine, rows, :] = (values * inverse * gain[...]).astype(BF16)
        return 0

    lax.fori_loop(0, 8, norm_rows, 0)
    csq[mine] = cs[...]

    pl.semaphore_wait(barrier, len(friends))

    rows = pl.ds(pl.multiple_of(col * 32, 32), 32)

    def pushes(n, what):
        r, slab, zl_, k_ = push_to[n]
        j = zl_ * 2 + k_
        index = r * 2 + k
        dev = device(slab, zl_, k_)
        narrow = pl.ds(pl.multiple_of(j * 128, 128), 128)
        wide = pl.ds(pl.multiple_of(j * 512, 512), 512)
        src, dst = (
            (kw.at[rows, narrow], wkv.at[index, rows, pl.ds(0, 128)]),
            (vw.at[rows, narrow], wkv.at[index, rows, pl.ds(128, 128)]),
            (qw.at[rows, wide], wq.at[index, rows, :]),
        )[what]
        return remote(src, dst, zs.at[n, what], zr.at[index - 2, what], dev)

    def pulled(i, what):
        dst = (wkv.at[2 + i, rows, pl.ds(0, 128)], wkv.at[2 + i, rows, pl.ds(128, 128)], wq.at[2 + i, rows, :])[what]
        return remote(dst, dst, zs.at[0, what], zr.at[i, what], core)

    for what in (0, 1, 2):
        for n in range(6):
            pushes(n, what).start()

    other = zl * 2 + (1 - k)
    to_core = [
        remote(kw.at[:, pl.ds(pl.multiple_of(other * 128, 128), 128)], wkv.at[k, :, pl.ds(0, 128)], ws.at[0], wr.at[0], core),
        remote(vw.at[:, pl.ds(pl.multiple_of(other * 128, 128), 128)], wkv.at[k, :, pl.ds(128, 128)], ws.at[1], wr.at[1], core),
        remote(qw.at[:, pl.ds(pl.multiple_of(other * 512, 512), 512)], wq.at[k], ws.at[2], wr.at[2], core),
        remote(tq.at[mine], tq.at[mine], ws.at[3], wr.at[3], core),
        remote(cs, csq.at[mine], ws.at[4], wr.at[4], core),
    ]
    for copy in to_core:
        copy.start()

    def quarter(q, i):
        return tq.at[q, :, pl.ds(i * 1024, 1024)]

    def to_chip(i):
        if i == 0:
            return remote(cs, csq.at[mine], ts.at[0], tr.at[0], chip)
        return remote(quarter(mine, i - 1), quarter(mine, i - 1), ts.at[i], tr.at[i], chip)

    theirs = k * 2 + (1 - zl)

    def from_chip(i):
        ref = csq.at[theirs] if i == 0 else quarter(theirs, i - 1)
        return remote(ref, ref, ts.at[i], tr.at[i], chip)

    def onward(i):
        ref = csq.at[theirs] if i == 0 else quarter(theirs, i - 1)
        return remote(ref, ref, fs.at[i], fr.at[i], core)

    far = (1 - k) * 2 + (1 - zl)

    def handed(i):
        ref = csq.at[far] if i == 0 else quarter(far, i - 1)
        return remote(ref, ref, fs.at[i], fr.at[i], core)

    for i in range(5):
        to_chip(i).start()

    wkv_g = PlaneGather(at, lambda g, h, p: wkv.at[pl.ds(2 + 3 * g, 3), pl.ds(pl.multiple_of(p * 32 + 16 * h, 16), 16), :],
                        s_a, r_a)
    wq_g = PlaneGather(at, lambda g, h, p: wq.at[pl.ds(2 + 3 * g, 3), pl.ds(pl.multiple_of(p * 32 + 16 * h, 16), 16), :],
                       s_b, r_b)
    kv_g = PlaneGather(at, lambda g, h, p: kvb.at[g, p, h], s_c, r_c)

    for i in range(6):
        pulled(i, 0).wait_recv()
        pulled(i, 1).wait_recv()
    for g in (0, 1):
        wkv_g.s0(g)
    for i in range(6):
        pulled(i, 2).wait_recv()
    for g in (0, 1):
        wq_g.s0(g)
    for g in (0, 1):
        wkv_g.s1(g)
    for g in (0, 1):
        wkv_g.s2(g)
    for g in (0, 1):
        wq_g.s1(g)

    def s3_kv(n, _):
        for g in (0, 1):
            wkv_g.s3(g, n)
        return 0

    lax.fori_loop(0, 4, s3_kv, 0)
    for g in (0, 1):
        wq_g.s2(g)

    def s4_kv(n, _):
        for g in (0, 1):
            wkv_g.s4(g, n)
        return 0

    lax.fori_loop(0, 4, s4_kv, 0)

    def s3_q(n, _):
        for g in (0, 1):
            wq_g.s3(g, n)
        return 0

    for i in range(5):
        if i < 2:
            from_chip(i).wait_recv()
            onward(i).start()
    lax.fori_loop(0, 2, s3_q, 0)
    for i in (2, 3):
        from_chip(i).wait_recv()
        onward(i).start()
    lax.fori_loop(2, 4, s3_q, 0)
    from_chip(4).wait_recv()
    onward(4).start()
    for copy in own:
        copy.wait()
    for copy in to_core:
        copy.wait_recv()
    for i in range(5):
        handed(i).wait_recv()

    def features(r):
        start = pl.multiple_of(lax.rem(zh + r, 4) * 1024, 1024)
        return tq[:, :, pl.ds(start, 1024)].reshape(512, 1024)

    def project_kv(r, _):
        w = wkv[pl.ds(2 * r, 2)].reshape(1024, 256)
        part = jnp.dot(features(r), w, preferred_element_type=F32)

        @pl.when(r == 0)
        def _():
            proj[:, 0:256] = part

        @pl.when(r > 0)
        def _():
            proj[:, 0:256] = proj[:, 0:256] + part

        return 0

    lax.fori_loop(0, 4, project_kv, 0)
    lane = lax.broadcasted_iota(jnp.int32, (1, 128), 1)
    offset = lax.rem(lane, 64).astype(F32)
    for g in (0, 1):
        for h in (0, 1):
            i = g * 2 + h
            key = rotate(proj[pl.ds(i * 128, 128), 0:128], csq[i, 0:128, :])
            kvb[g, col, h, 0:128, :] = key.astype(BF16)
            kvb[g, col, h, 128:256, :] = proj[pl.ds(i * 128, 128), 128:256].T.astype(BF16)
            block = (csq[i, 128:129, :] - offset) * (1.0 / 64.0)
            line = lax.broadcasted_iota(jnp.int32, (16, 128), 0)
            kvb[g, col, h, 256:272, :] = jnp.where(line == 0, jnp.broadcast_to(block, (16, 128)), 1.0).astype(BF16)
    for g in (0, 1):
        kv_g.s0(g)

    def s4_q(n, _):
        for g in (0, 1):
            wq_g.s4(g, n)
        return 0

    lax.fori_loop(0, 4, s4_q, 0)

    def project_q(r, _):
        w = wq[pl.ds(2 * r, 2)].reshape(1024, 512)
        part = jnp.dot(features(r), w, preferred_element_type=F32)

        @pl.when(r == 0)
        def _():
            proj[...] = part

        @pl.when(r > 0)
        def _():
            proj[...] = proj[...] + part

        return 0

    lax.fori_loop(0, 4, project_q, 0)
    for g in (0, 1):
        kv_g.s1(g)
    for i in range(4):
        for hd in range(GROUP):
            u = rotate(proj[pl.ds(i * 128, 128), pl.ds(hd * 128, 128)], csq[i, 0:128, :])
            at_col = ((i % 2) * GROUP + hd) * 128
            qt[i // 2, :, at_col:at_col + 128] = u.T.astype(BF16)
    acc[...] = jnp.zeros_like(acc)
    top[...] = jnp.full_like(top, FLOOR)

    scale = HEAD ** -0.5 * LOG2E
    within = lax.rem(lax.broadcasted_iota(jnp.int32, (128, 128), 0), 64).astype(F32)
    upper = lax.broadcasted_iota(jnp.int32, (128, 128), 0) < 64

    def attend(g, slots):
        keys, values, spots = [], [], []
        for p in slots:
            for h in (0, 1):
                keys.append(kvb[g, p, h, 0:128, :])
                values.append(kvb[g, p, h, 128:272, :])
                block = kvb[g, p, h, 256:272, :].astype(F32)[0:1, :]
                spots.append(jnp.where(upper, block[:, 0:1], block[:, 64:65]) * 64.0 + within)
        keys = jnp.concatenate(keys, axis=0)
        values = jnp.concatenate(values, axis=1)
        spots = jnp.concatenate(spots, axis=0)
        spots = jnp.concatenate([spots, spots], axis=1)
        for tile in range(4):
            cols = slice(tile * 256, tile * 256 + 256)
            place = csq[g * 2 + tile // 2, 128:129, :]
            place = jnp.concatenate([place, place], axis=1)
            scores = jnp.dot(keys, qt[g, :, cols], preferred_element_type=F32)
            scores = jnp.where(spots <= place, scores, FLOOR)
            before = top[g, 0:1, cols]
            now = jnp.maximum(before, jnp.max(scores, axis=0, keepdims=True))
            probs = jnp.exp2((scores - now) * scale).astype(BF16)
            factor = jnp.exp2((before - now) * scale)
            acc[g, :, cols] = acc[g, :, cols] * factor + jnp.dot(values, probs, preferred_element_type=F32)
            top[g, 0:1, cols] = now

    def round_(i, _):
        @pl.when(i == 1)
        def _():
            for g in (0, 1):
                kv_g.s2(g)

        @pl.when((i >= 2) & (i < 6))
        def _():
            for g in (0, 1):
                kv_g.s3(g, i - 2)

        @pl.when(i >= 6)
        def _():
            for g in (0, 1):
                kv_g.s4(g, (i - 6) * 2)
                kv_g.s4(g, (i - 6) * 2 + 1)

        n = lax.rem(i, 2) * 2
        da0 = around(jnp.where(i < 2, n, jnp.where(i < 6, i - 2, n)))
        da1 = around(jnp.where(i < 2, n + 1, jnp.where(i < 6, i - 2, n + 1)))
        db0 = jnp.where(i < 2, 0, jnp.where(i < 6, 3, 2))
        db1 = jnp.where(i < 2, 0, jnp.where(i < 6, 1, 2))
        for g in (0, 1):
            attend(g, (kv_g.slot(g, da0, db0), kv_g.slot(g, da1, db1)))
        return 0

    lax.fori_loop(0, 8, round_, 0)

    for g in (0, 1):
        for h in (0, 1):
            for hd in range(GROUP):
                at_col = (h * GROUP + hd) * 128
                one = acc[g, 0:128, at_col:at_col + 128] / acc[g, 129:130, at_col:at_col + 128]
                osend[g * 2 + h, :, hd * 128:hd * 128 + 128] = one.T.astype(BF16)

    def give(n):
        g, h, dev = ((k, 1 - zl, chip), (1 - k, 1 - zl, diagonal), (1 - k, zl, core))[n]
        return remote(osend.at[g * 2 + h], obuf.at[head], os_.at[n], or_.at[n], dev)

    def take(n):
        j = ((1 - zl) * 2 + k, (1 - zl) * 2 + 1 - k, zl * 2 + 1 - k)[n]
        return j, remote(obuf.at[j], obuf.at[j], os_.at[n], or_.at[n], core)

    for n in range(3):
        give(n).start()

    def store(src, j, n):
        return pltpu.make_async_copy(src, out.at[:, pl.ds(pl.multiple_of(j * 512, 512), 512)], outs_.at[n])

    last = [store(osend.at[mine], head, 3)]
    last[0].start()
    for n in (2, 0, 1):
        j, arrival = take(n)
        arrival.wait_recv()
        last.append(store(obuf.at[j], j, n))
        last[-1].start()
    for n in range(6):
        for what in (0, 1, 2):
            pushes(n, what).wait_send()
    for copy in to_core:
        copy.wait_send()
    for i in range(5):
        to_chip(i).wait_send()
        onward(i).wait_send()
    for gather in (wkv_g, wq_g, kv_g):
        gather.finish()
    for n in range(3):
        give(n).wait_send()
    for copy in last:
        copy.wait()


def on_device(tokens, positions, norm_gain, query_weight, key_weight, value_matrix):
    places = positions[0]
    table = jnp.concatenate([rope_tables(places), jnp.broadcast_to(places.astype(F32)[None, :], (8, 128))], axis=0)
    vmem = pl.BlockSpec(memory_space=pltpu.VMEM)
    anywhere = pl.BlockSpec(memory_space=pl.ANY)
    dma = pltpu.SemaphoreType.DMA
    result = pl.pallas_call(
        kernel,
        out_shape=jax.ShapeDtypeStruct((128, 2048), BF16),
        in_specs=[vmem, vmem, vmem, anywhere, anywhere, anywhere],
        out_specs=anywhere,
        scratch_shapes=[
            pltpu.VMEM((4, 128, 4096), BF16),
            pltpu.VMEM((4, 136, 128), F32),
            pltpu.VMEM((8, 512, 256), BF16),
            pltpu.VMEM((8, 512, 512), BF16),
            pltpu.VMEM((2, 16, 2, 272, 128), BF16),
            pltpu.VMEM((2, 128, 1024), BF16),
            pltpu.VMEM((2, 144, 1024), F32),
            pltpu.VMEM((2, 8, 1024), F32),
            pltpu.VMEM((512, 512), F32),
            pltpu.VMEM((4, 128, 512), BF16),
            pltpu.VMEM((4, 128, 512), BF16),
            dma((3,)), dma((6, 3)), dma((6, 3)), dma((5,)), dma((5,)), dma((5,)), dma((5,)), dma((5,)), dma((5,)),
            dma((2, 30)), dma((2, 16, 2)), dma((2, 30)), dma((2, 16, 2)), dma((2, 30)), dma((2, 16, 2)),
            dma((3,)), dma((3,)), dma((4,)),
        ],
        compiler_params=pltpu.CompilerParams(
            collective_id=0, has_side_effects=True, vmem_limit_bytes=56 * 1024 * 1024),
    )(tokens[0], norm_gain[None, :], table, query_weight, key_weight, value_matrix)
    return result[None]


def solution(mesh):
    placed = (
        P("fsdp", "ctx", None),
        P("fsdp", "ctx"),
        P(),
        P("fsdp", None),
        P("fsdp", None),
        P("fsdp", None),
    )
    return jax.shard_map(
        on_device, mesh=mesh, in_specs=placed, out_specs=P("fsdp", "ctx", None), check_vma=False
    )
```

```python
import math

import jax
import jax.numpy as jnp
from jax import lax
from jax.experimental import pallas as pl
from jax.experimental.pallas import tpu as pltpu
from jax.sharding import PartitionSpec as P

HEAD = 128
GROUP = 4
EPS = 1e-05
BASE = 500000.0
FLOOR = -1e30
LOG2E = math.log2(math.e)
F32, BF16 = jnp.float32, jnp.bfloat16


def rope_tables(places):
    half = HEAD // 2
    frequency = BASE ** (-(jnp.arange(half, dtype=F32) * 2.0) / HEAD)
    angles = places.astype(F32)[:, None] * frequency[None, :]
    return jnp.concatenate([jnp.cos(angles), jnp.sin(angles)], axis=1)


def around(n):
    return jnp.where(n == 0, 0, jnp.where(n == 1, 3, jnp.where(n == 2, 1, 2)))


class PlaneGather:
    def __init__(self, at, piece, sems, shared, sent):
        self.at, self.piece, self.sent = at, piece, sent
        self.send_sem, self.recv_sem, self.rest_sem, self.shared = *sems, shared

    def slot(self, g, da, db):
        dx, dy = (da, db) if g == 0 else (db, da)
        return lax.rem(self.at["x"] + dx, 4) * 4 + lax.rem(self.at["y"] + dy, 4)

    def neighbour(self, g, axis, step):
        along_x = (axis == 0) == (g == 0)
        dx, dy = (step, 0) if along_x else (0, step)
        ctx = self.at["zl"] * 16 + lax.rem(self.at["x"] + dx, 4) * 4 + lax.rem(self.at["y"] + dy, 4)
        return {"ctx": ctx, "fsdp": self.at["f"]}

    def early(self, g, d, h):
        return self.recv_sem.at[g, (0, 2, 4, 0)[d] + h] if d != 1 else self.recv_sem.at[g, 2 + h]

    def relayed(self, g, n, h):
        return self.recv_sem.at[g, 6 + n * 2 + h]

    def rest(self, n, h):
        return self.rest_sem.at[self.shared(n, h)]

    def copy(self, g, h, p, recv_sem, device):
        ref = self.piece(g, h, p)
        return pltpu.make_async_remote_copy(
            src_ref=ref, dst_ref=ref, send_sem=self.send_sem.at[min(h, self.send_sem.shape[0] - 1)], recv_sem=recv_sem,
            device_id=device, device_id_type=pl.DeviceIdType.MESH)

    def send(self, g, h, p, recv_sem, axis, step):
        self.copy(g, h, p, recv_sem, self.neighbour(g, axis, step)).start()

    def arrived(self, g, h, p, recv_sem):
        self.copy(g, h, p, recv_sem, self.neighbour(g, 0, 1)).wait_recv()

    def first(self, g):
        p = self.slot(g, 0, 0)
        for h in (0, 1):
            self.send(g, h, p, self.early(g, 3, h), 0, 1)
            self.send(g, h, p, self.early(g, 1, h), 0, 3)

    def second(self, g, n, da):
        p = self.slot(g, da, 0)
        for h in (0, 1):
            self.send(g, h, p, self.rest(n, h) if h else self.relayed(g, n, 0), 1, 1)
            self.send(g, h, p, self.relayed(g, n, 1) if h else self.rest(n, h), 1, 3)

    def relay(self, g):
        for d, h, step in ((3, 0, 1), (1, 1, 3)):
            p = self.slot(g, d, 0)
            self.arrived(g, h, p, self.early(g, d, h))
            self.send(g, h, p, self.early(g, 2, h), 0, step)

    def s1(self, g):
        for n, d, h in ((1, 3, 1), (2, 1, 0)):
            self.arrived(g, h, self.slot(g, d, 0), self.early(g, d, h))
            self.second(g, n, d)

    def s2(self, g):
        p = self.slot(g, 2, 0)
        for h in (0, 1):
            self.arrived(g, h, p, self.early(g, 2, h))
        self.second(g, 3, 2)

    def s3(self, g, n):
        d = around(n)
        for db, h, step in ((3, 0, 1), (1, 1, 3)):
            p = self.slot(g, d, db)
            self.arrived(g, h, p, self.relayed(g, n, h))
            self.send(g, h, p, self.rest(4, h), 1, step)

    def gathered(self, ref, sem):
        pltpu.make_async_copy(ref, ref, sem).wait()

    def finish(self):
        for h, ref in enumerate(self.sent):
            self.gathered(ref, self.send_sem.at[h])


def rotate(u, table):
    turned = pltpu.roll(table, 64, 1)
    first = lax.broadcasted_iota(jnp.int32, table.shape, 1) < 64
    cosine = jnp.where(first, table, turned)
    sine = jnp.where(first, -turned, table)
    return u * cosine + pltpu.roll(u, 64, 1) * sine


def kernel(tok_in, gain, cs, qw, kw, vw, out,
           tok, rq, rk, rv, tq, csq, wkv, wq, kb, vb, qt, acc, top, proj, sbuf, osend, obuf,
           tok_s, loc_s, zs, zr, ws, wr, ts, tr, fs, fr,
           s_a, r_a, x_a, s_b, r_b, x_b, s_c, r_c, x_c, s_d, r_d, x_d, os_, or_, outs_):
    c, f = lax.axis_index("ctx"), lax.axis_index("fsdp")
    zl, x, y = c // 16, lax.rem(c // 4, 4), lax.rem(c, 4)
    zh, k = f // 2, lax.rem(f, 2)
    col = x * 4 + y
    at = {"zl": zl, "x": x, "y": y, "f": f}
    head = zl * 2 + k

    def device(zh_, zl_, k_):
        return {"ctx": zl_ * 16 + col, "fsdp": zh_ * 2 + k_}

    def remote(src, dst, ss, rs, dev):
        return pltpu.make_async_remote_copy(src_ref=src, dst_ref=dst, send_sem=ss, recv_sem=rs, device_id=dev,
                                            device_id_type=pl.DeviceIdType.MESH)

    core = device(zh, zl, 1 - k)
    chip = device(zh, 1 - zl, k)
    diagonal = device(zh, 1 - zl, 1 - k)
    step_a = 1 + 2 * zl
    slab_a = lax.rem(zh + 4 - step_a, 4)
    slab_c = lax.rem(zh + step_a, 4)
    slab_b = lax.rem(zh + 2, 4)
    push_to = [(step_a, slab_a, zl_, k_) for zl_ in (0, 1) for k_ in (0, 1)] + [(2, slab_b, 1 - zl, k_) for k_ in (0, 1)]

    barrier = pltpu.get_barrier_semaphore()
    ring = PlaneGather(at, None, (None, None, None), None, None)
    friends = [device(slab_b, 1 - zl, k_) for k_ in (0, 1)]
    friends += [device(slab_a, zl_, k_) for zl_ in (0, 1) for k_ in (0, 1)]
    friends += [device(slab_c, zl, k_) for k_ in (0, 1)]
    friends += [core, chip, diagonal]
    friends += [ring.neighbour(0, axis, step) for axis in (0, 1) for step in (1, 3)]
    for friend in friends:
        pl.semaphore_signal(barrier, inc=1, device_id=friend, device_id_type=pl.DeviceIdType.MESH)

    rows = pl.ds(pl.multiple_of(col * 32, 32), 32)
    loads = [pltpu.make_async_copy(tok_in.at[pl.ds(i * 64, 64), :], tok.at[pl.ds(i * 64, 64), :], tok_s.at[i]) for i in (0, 1)]
    staged = [pltpu.make_async_copy(src.at[rows, :], dst, tok_s.at[2 + i])
              for i, (src, dst) in enumerate(((kw, rk), (vw, rv), (qw, rq)))]
    own = [
        pltpu.make_async_copy(kw.at[:, pl.ds(pl.multiple_of(head * 128, 128), 128)], wkv.at[k, :, pl.ds(0, 128)], loc_s.at[0]),
        pltpu.make_async_copy(vw.at[:, pl.ds(pl.multiple_of(head * 128, 128), 128)], wkv.at[k, :, pl.ds(128, 128)], loc_s.at[1]),
        pltpu.make_async_copy(qw.at[:, pl.ds(pl.multiple_of(head * 512, 512), 512)], wq.at[k], loc_s.at[2]),
    ]
    for copy in loads + staged + own:
        copy.start()

    def norm_rows(i, _):
        line = pl.ds(pl.multiple_of(i * 16, 16), 16)
        values = tok[line, :].astype(F32)
        inverse = lax.rsqrt(jnp.mean(values * values, axis=-1, keepdims=True) + EPS)
        tq[k, line, :] = (values * inverse * gain[...]).astype(BF16)
        return 0

    for i, copy in enumerate(loads):
        copy.wait()
        lax.fori_loop(i * 4, i * 4 + 4, norm_rows, 0)
    csq[k] = cs[...]
    for copy in staged:
        copy.wait()

    pl.semaphore_wait(barrier, len(friends))

    def pushes(n, what):
        r, slab, zl_, k_ = push_to[n]
        j = zl_ * 2 + k_
        index = r * 2 + k
        dev = device(slab, zl_, k_)
        narrow = pl.ds(pl.multiple_of(j * 128, 128), 128)
        wide = pl.ds(pl.multiple_of(j * 512, 512), 512)
        src, dst = (
            (rk.at[:, narrow], wkv.at[index, rows, pl.ds(0, 128)]),
            (rv.at[:, narrow], wkv.at[index, rows, pl.ds(128, 128)]),
            (rq.at[:, wide], wq.at[index, rows, :]),
        )[what]
        return remote(src, dst, zs.at[what // 2], zr.at[what // 2], dev)

    def whole(ref, sem):
        pltpu.make_async_copy(ref, ref, sem).wait()

    for n in (4, 5, 0, 1, 2, 3):
        pushes(n, 0).start()
        pushes(n, 1).start()
    for n in (4, 5, 0, 1, 2, 3):
        pushes(n, 2).start()

    other = zl * 2 + (1 - k)
    to_core = [
        remote(kw.at[:, pl.ds(pl.multiple_of(other * 128, 128), 128)], wkv.at[k, :, pl.ds(0, 128)], ws.at[0], wr.at[0], core),
        remote(vw.at[:, pl.ds(pl.multiple_of(other * 128, 128), 128)], wkv.at[k, :, pl.ds(128, 128)], ws.at[1], wr.at[1], core),
        remote(qw.at[:, pl.ds(pl.multiple_of(other * 512, 512), 512)], wq.at[k], ws.at[2], wr.at[2], core),
        remote(tq.at[k], tq.at[k], ws.at[3], wr.at[3], core),
        remote(cs, csq.at[k], ws.at[4], wr.at[4], core),
    ]
    for copy in to_core:
        copy.start()

    def quarter(q, i):
        return tq.at[q, :, pl.ds(i * 1024, 1024)]

    def to_chip(i):
        if i == 0:
            return remote(cs, csq.at[2 + k], ts.at[0], tr.at[0], chip)
        return remote(quarter(k, i - 1), quarter(2 + k, i - 1), ts.at[i], tr.at[i], chip)

    def from_chip(i):
        ref = csq.at[2 + k] if i == 0 else quarter(2 + k, i - 1)
        return remote(ref, ref, ts.at[i], tr.at[i], chip)

    def onward(i):
        ref = csq.at[2 + k] if i == 0 else quarter(2 + k, i - 1)
        return remote(ref, ref, fs.at[i], fr.at[i], core)

    def handed(i):
        ref = csq.at[3 - k] if i == 0 else quarter(3 - k, i - 1)
        return remote(ref, ref, fs.at[i], fr.at[i], core)

    for i in range(5):
        to_chip(i).start()

    def pass_on(*which):
        for i in which:
            from_chip(i).wait_recv()
            onward(i).start()

    def pieces(w):
        return lambda g, h, p: w.at[pl.ds(2 + 3 * g, 3), pl.ds(pl.multiple_of(p * 32 + 16 * h, 16), 16), :]

    wkv_g = PlaneGather(at, pieces(wkv), (s_a, r_a, x_a), lambda n, h: 0, (wkv.at[0:6, 0:480],))
    wq_g = PlaneGather(at, pieces(wq), (s_b, r_b, x_b), lambda n, h: 0, (wq.at[0:6, 0:480],))
    kv_g = [PlaneGather(at, lambda g, h, p, m=m: vb.at[g, p, m] if h else kb.at[g, p, m], sems, lambda n, h: n * 2 + h,
                        (kb.at[:, 0:15, 0], vb.at[:, 0:15, 0]))
            for m, sems in enumerate(((s_c, r_c, x_c), (s_d, r_d, x_d)))]

    def kv_third(m, n):
        whole(kb.at[:, 0, 0], kv_g[m].rest(n, 0))
        whole(vb.at[:, 0, 0], kv_g[m].rest(n, 1))

    def kv_fourth(m):
        whole(kb.at[:, 0:4, 0], kv_g[m].rest(4, 0))
        whole(vb.at[:, 0:4, 0], kv_g[m].rest(4, 1))

    def both(step):
        for g in (0, 1):
            step(g)

    def each(step, lo, hi):
        def body(n, _):
            for g in (0, 1):
                step(g, n)
            return 0

        lax.fori_loop(lo, hi, body, 0)

    def third(gather, n):
        for g in (0, 1):
            gather.s3(g, n)

    def sideways(gather):
        for g in (0, 1):
            gather.second(g, 0, 0)

    def features(lo, count, r):
        start = pl.multiple_of(lax.rem(zh + r, 4) * 1024, 1024)
        return tq[lo:lo + count, :, pl.ds(start, 1024)].reshape(count * 128, 1024)

    lane = lax.broadcasted_iota(jnp.int32, (1, 128), 1)
    offset = lax.rem(lane, 64).astype(F32)

    def accumulate(r, lo, count, w, width):
        part = jnp.dot(features(lo, count, r), w, preferred_element_type=F32)
        size = count * 128

        @pl.when(r == 0)
        def _():
            proj[0:size, 0:width] = part

        @pl.when(r > 0)
        def _():
            proj[0:size, 0:width] = proj[0:size, 0:width] + part

    def make_kv(m):
        def project(r, _):
            accumulate(r, 2 * m, 2, wkv[pl.ds(2 * r, 2)].reshape(1024, 256), 256)
            return 0

        lax.fori_loop(0, 4, project, 0)
        for g in (0, 1):
            i = m * 2 + g
            key = rotate(proj[g * 128:g * 128 + 128, 0:128], csq[i, 0:128, :])
            kb[g, col, m, 0:128, :] = key.astype(BF16)
            vb[g, col, m] = proj[g * 128:g * 128 + 128, 128:256].T.astype(BF16)
            block = (csq[i, 128:129, :] - offset) * (1.0 / 64.0)
            kb[g, col, m, 128:144, :] = jnp.broadcast_to(block, (16, 128)).astype(BF16)

    def project_q(r, _):
        accumulate(r, 0, 4, wq[pl.ds(2 * r, 2)].reshape(1024, 512), 512)
        return 0

    whole(wkv.at[2:8, 0:32], zr.at[0])
    kv_a, kv_b = kv_g
    both(wkv_g.first)
    sideways(wkv_g)
    both(wkv_g.relay)
    both(wkv_g.s1)
    whole(wq.at[2:8, 0:32], zr.at[1])
    both(wq_g.first)
    both(wkv_g.s2)
    sideways(wq_g)
    third(wkv_g, 0)
    both(wq_g.relay)
    third(wkv_g, 1)
    third(wkv_g, 3)
    third(wkv_g, 2)
    both(wq_g.s1)
    whole(wkv.at[0:6, 0:256], x_a.at[0])
    both(wq_g.s2)
    own[0].wait()
    own[1].wait()
    for i in (0, 1, 3, 4):
        to_core[i].wait_recv()
    make_kv(0)
    both(kv_a.first)
    pass_on(0, 1, 2, 3)
    each(wq_g.s3, 0, 3)
    both(kv_a.relay)
    both(kv_a.s1)
    third(wq_g, 3)
    pass_on(4)
    for i in range(5):
        handed(i).wait_recv()
    make_kv(1)
    third(kv_a, 1)
    both(kv_b.first)
    both(kv_a.s2)
    sideways(kv_a)
    whole(wq.at[0:6, 0:256], x_b.at[0])
    own[2].wait()
    to_core[2].wait_recv()
    lax.fori_loop(0, 2, project_q, 0)
    third(kv_a, 2)
    both(kv_b.relay)
    third(kv_a, 3)
    both(kv_b.s1)
    third(kv_a, 0)
    lax.fori_loop(2, 4, project_q, 0)
    sideways(kv_b)

    edge = lax.broadcasted_iota(jnp.int32, (128, 128), 0)
    for i in range(4):
        block = (csq[i, 128:129, :] - offset) * (1.0 / 64.0)
        later = jnp.where(edge.astype(F32) > block, FLOOR, 0.0).astype(BF16)
        for hd in range(GROUP):
            u = rotate(proj[pl.ds(i * 128, 128), pl.ds(hd * 128, 128)], csq[i, 0:128, :])
            at_col = ((i // 2) * GROUP + hd) * 128
            qt[i % 2, 0:128, at_col:at_col + 128] = u.T.astype(BF16)
            qt[i % 2, 128:256, at_col:at_col + 128] = later
    acc[...] = jnp.zeros_like(acc)
    top[...] = jnp.full_like(top, FLOOR)
    both(kv_b.s2)

    scale = HEAD ** -0.5 * LOG2E
    upper = edge < 64
    across = lax.broadcasted_iota(jnp.int32, (128, 128), 1)
    triangle = jnp.where((edge > across) & ((edge < 64) == (across < 64)), FLOOR, 0.0)
    numbers = across.astype(F32)
    ones = jnp.ones((16, 512), BF16)

    def attend(i, halves):
        m, turn = i // 4, lax.rem(i, 4)
        ends = (turn == 0) | (turn == 3)
        slots = []
        for e in range(4):
            da = around(jnp.where(ends, e, 2 * (turn - 1) + e // 2))
            db = jnp.where(turn == 0, 0, jnp.where(turn == 3, 2, 3 - 2 * (e % 2)))
            slots.append((da, db))
        work = []
        for g in (0, 1):
            keys, values, runs = [], [], []
            for da, db in slots:
                p = kv_g[0].slot(g, da, db)
                keys.append(kb[g, p, m, 0:128, :])
                values.append(vb[g, p, m])
                block = kb[g, p, m, 128:144, :].astype(F32)[0:1, :]
                run = jnp.where(upper, block[:, 0:1], block[:, 64:65])
                runs.append(jnp.where(run == numbers, 1.0, 0.0).astype(BF16))
            keys = jnp.concatenate([jnp.concatenate(keys, axis=0), jnp.concatenate(runs, axis=0)], axis=1)
            values = jnp.concatenate([jnp.concatenate(values, axis=1), ones], axis=0)
            for half in halves:
                own_run = triangle * jnp.where((turn == 0) & (m == half), 1.0, 0.0)
                for tile in (0, 1):
                    work.append((g, keys, values, own_run, pl.ds(pl.multiple_of(half * 512 + tile * 256, 256), 256)))

        def score(t):
            g, keys, _, own_run, cols = work[t]
            scores = jnp.dot(keys, qt[g, :, cols], preferred_element_type=F32)
            first = scores[0:128] + jnp.concatenate([own_run, own_run], axis=1)
            sbuf[t % 2, 0:128] = first
            sbuf[t % 2, 128:512] = scores[128:512]
            return jnp.maximum(jnp.max(first, axis=0, keepdims=True), jnp.max(scores[128:512], axis=0, keepdims=True))

        best = score(0)
        for t in range(len(work)):
            g, _, values, _, cols = work[t]
            following = score(t + 1) if t + 1 < len(work) else None
            before = top[g, 0:1, cols]
            now = jnp.maximum(before, best)
            probs = jnp.exp2((sbuf[t % 2] - now) * scale).astype(BF16)
            factor = jnp.exp2((before - now) * scale)
            acc[g, :, cols] = acc[g, :, cols] * factor + jnp.dot(values, probs, preferred_element_type=F32)
            top[g, 0:1, cols] = now
            best = following

    def settle(m):
        for g in (0, 1):
            for hd in range(GROUP):
                at_col = m * 512 + hd * 128
                one = acc[g, 0:128, at_col:at_col + 128] / acc[g, 128:129, at_col:at_col + 128]
                osend[m * 2 + g, :, hd * 128:hd * 128 + 128] = one.T.astype(BF16)

    def give(n):
        src, dev = ((2 + k, chip), (3 - k, diagonal), (1 - k, core))[n]
        return remote(osend.at[src], obuf.at[head], os_.at[n], or_.at[n], dev)

    def take(n):
        j = ((1 - zl) * 2 + k, (1 - zl) * 2 + 1 - k, zl * 2 + 1 - k)[n]
        return j, remote(obuf.at[j], obuf.at[j], os_.at[n], or_.at[n], core)

    def round_both(i, _):
        @pl.when(i == 1)
        def _():
            third(kv_b, 1)
            kv_third(0, 0)
            kv_third(0, 1)

        @pl.when(i == 2)
        def _():
            third(kv_b, 2)
            kv_third(0, 2)
            kv_third(0, 3)

        @pl.when(i == 3)
        def _():
            kv_fourth(0)
            third(kv_b, 0)

        attend(i, (1, 0))
        return 0

    def round_one(step, _):
        @pl.when(step == 0)
        def _():
            third(kv_b, 3)

        @pl.when(step == 1)
        def _():
            kv_third(1, 0)
            kv_third(1, 1)

        @pl.when(step == 2)
        def _():
            kv_third(1, 2)
            kv_third(1, 3)

        @pl.when(step == 3)
        def _():
            kv_fourth(1)

        @pl.when(step == 4)
        def _():
            settle(1)
            give(0).start()
            give(1).start()

        attend(4 + lax.rem(step, 4), (jnp.where(step < 4, 1, 0),))
        return 0

    lax.fori_loop(0, 4, round_both, 0)
    lax.fori_loop(0, 8, round_one, 0)
    settle(0)
    give(2).start()

    def store(src, j, n):
        return pltpu.make_async_copy(src, out.at[:, pl.ds(pl.multiple_of(j * 512, 512), 512)], outs_.at[n])

    last = [store(osend.at[k], head, 3)]
    last[0].start()
    whole(wkv.at[2:8, 0:32], zs.at[0])
    whole(wq.at[2:8, 0:32], zs.at[1])
    for copy in to_core:
        copy.wait_send()
    for i in range(5):
        to_chip(i).wait_send()
        onward(i).wait_send()
    for gather in (wkv_g, wq_g, kv_g[0], kv_g[1]):
        gather.finish()
    for n in (2, 0, 1):
        j, arrival = take(n)
        arrival.wait_recv()
        last.append(store(obuf.at[j], j, n))
        last[-1].start()
    for n in range(3):
        give(n).wait_send()
    for copy in last:
        copy.wait()


def on_device(tokens, positions, norm_gain, query_weight, key_weight, value_matrix):
    places = positions[0]
    table = jnp.concatenate([rope_tables(places), jnp.broadcast_to(places.astype(F32)[None, :], (8, 128))], axis=0)
    vmem = pl.BlockSpec(memory_space=pltpu.VMEM)
    anywhere = pl.BlockSpec(memory_space=pl.ANY)
    far = pl.BlockSpec(memory_space=pltpu.HBM)
    dma = pltpu.SemaphoreType.DMA
    result = pl.pallas_call(
        kernel,
        out_shape=jax.ShapeDtypeStruct((128, 2048), BF16),
        in_specs=[far, vmem, vmem, far, far, far],
        out_specs=anywhere,
        scratch_shapes=[
            pltpu.VMEM((128, 4096), BF16),
            pltpu.VMEM((32, 2048), BF16),
            pltpu.VMEM((32, 512), BF16),
            pltpu.VMEM((32, 512), BF16),
            pltpu.VMEM((4, 128, 4096), BF16),
            pltpu.VMEM((4, 136, 128), F32),
            pltpu.VMEM((8, 512, 256), BF16),
            pltpu.VMEM((8, 512, 512), BF16),
            pltpu.VMEM((2, 16, 2, 144, 128), BF16),
            pltpu.VMEM((2, 16, 2, 128, 128), BF16),
            pltpu.VMEM((2, 256, 1024), BF16),
            pltpu.VMEM((2, 144, 1024), F32),
            pltpu.VMEM((2, 8, 1024), F32),
            pltpu.VMEM((512, 512), F32),
            pltpu.VMEM((2, 512, 256), F32),
            pltpu.VMEM((4, 128, 512), BF16),
            pltpu.VMEM((4, 128, 512), BF16),
            dma((5,)), dma((3,)), dma((2,)), dma((2,)), dma((5,)), dma((5,)), dma((5,)), dma((5,)), dma((5,)), dma((5,)),
            dma((1,)), dma((2, 14)), dma((1,)), dma((1,)), dma((2, 14)), dma((1,)),
            dma((2,)), dma((2, 14)), dma((10,)), dma((2,)), dma((2, 14)), dma((10,)),
            dma((3,)), dma((3,)), dma((4,)),
        ],
        compiler_params=pltpu.CompilerParams(
            collective_id=0, has_side_effects=True, vmem_limit_bytes=53 * 1024 * 1024),
    )(tokens[0], norm_gain[None, :], table, query_weight, key_weight, value_matrix)
    return result[None]


def solution(mesh):
    placed = (
        P("fsdp", "ctx", None),
        P("fsdp", "ctx"),
        P(),
        P("fsdp", None),
        P("fsdp", None),
        P("fsdp", None),
    )
    return jax.shard_map(
        on_device, mesh=mesh, in_specs=placed, out_specs=P("fsdp", "ctx", None), check_vma=False
    )
```

```python
import math

import jax
import jax.numpy as jnp
from jax import lax
from jax.experimental import pallas as pl
from jax.experimental.pallas import tpu as pltpu
from jax.sharding import PartitionSpec as P

HEAD = 128
GROUP = 4
EPS = 1e-05
BASE = 500000.0
FLOOR = -1e30
LOG2E = math.log2(math.e)
F32, BF16 = jnp.float32, jnp.bfloat16


def around(n):
    return jnp.where(n == 0, 0, jnp.where(n == 1, 3, jnp.where(n == 2, 1, 2)))


class PlaneGather:
    def __init__(self, at, piece, sems, shared, sent):
        self.at, self.piece, self.sent = at, piece, sent
        self.send_sem, self.recv_sem, self.rest_sem, self.shared = *sems, shared

    def slot(self, g, da, db):
        if isinstance(g, int):
            dx, dy = (da, db) if g == 0 else (db, da)
        else:
            dx, dy = jnp.where(g == 0, da, db), jnp.where(g == 0, db, da)
        return lax.rem(self.at["x"] + dx, 4) * 4 + lax.rem(self.at["y"] + dy, 4)

    def neighbour(self, g, axis, step):
        along_x = (axis == 0) == (g == 0)
        dx, dy = (step, 0) if along_x else (0, step)
        ctx = self.at["zl"] * 16 + lax.rem(self.at["x"] + dx, 4) * 4 + lax.rem(self.at["y"] + dy, 4)
        return {"ctx": ctx, "fsdp": self.at["f"]}

    def early(self, g, d, h):
        return self.recv_sem.at[g, (0, 2, 4, 0)[d] + h] if d != 1 else self.recv_sem.at[g, 2 + h]

    def relayed(self, g, n, h):
        return self.recv_sem.at[g, 6 + n * 2 + h]

    def rest(self, n, h):
        return self.rest_sem.at[self.shared(n, h)]

    def copy(self, g, h, p, recv_sem, device):
        ref = self.piece(g, h, p)
        return pltpu.make_async_remote_copy(
            src_ref=ref, dst_ref=ref, send_sem=self.send_sem.at[min(h, self.send_sem.shape[0] - 1)], recv_sem=recv_sem,
            device_id=device, device_id_type=pl.DeviceIdType.MESH)

    def send(self, g, h, p, recv_sem, axis, step):
        self.copy(g, h, p, recv_sem, self.neighbour(g, axis, step)).start()

    def arrived(self, g, h, p, recv_sem):
        self.copy(g, h, p, recv_sem, self.neighbour(g, 0, 1)).wait_recv()

    def first(self, g):
        p = self.slot(g, 0, 0)
        for h in (0, 1):
            self.send(g, h, p, self.early(g, 3, h), 0, 1)
            self.send(g, h, p, self.early(g, 1, h), 0, 3)

    def second(self, g, n, da):
        p = self.slot(g, da, 0)
        for h in (0, 1):
            self.send(g, h, p, self.rest(n, h) if h else self.relayed(g, n, 0), 1, 1)
            self.send(g, h, p, self.relayed(g, n, 1) if h else self.rest(n, h), 1, 3)

    def relay(self, g):
        for d, h, step in ((3, 0, 1), (1, 1, 3)):
            p = self.slot(g, d, 0)
            self.arrived(g, h, p, self.early(g, d, h))
            self.send(g, h, p, self.early(g, 2, h), 0, step)

    def s1(self, g):
        for n, d, h in ((1, 3, 1), (2, 1, 0)):
            self.arrived(g, h, self.slot(g, d, 0), self.early(g, d, h))
            self.second(g, n, d)

    def s2(self, g):
        p = self.slot(g, 2, 0)
        for h in (0, 1):
            self.arrived(g, h, p, self.early(g, 2, h))
        self.second(g, 3, 2)

    def s3(self, g, n):
        d = around(n)
        for db, h, step in ((3, 0, 1), (1, 1, 3)):
            p = self.slot(g, d, db)
            self.arrived(g, h, p, self.relayed(g, n, h))
            self.send(g, h, p, self.rest(4, h), 1, step)

    def gathered(self, ref, sem):
        pltpu.make_async_copy(ref, ref, sem).wait()

    def finish(self):
        for h, ref in enumerate(self.sent):
            self.gathered(ref, self.send_sem.at[h])


def rotate(u, table):
    turned = pltpu.roll(table, 64, 1)
    first = lax.broadcasted_iota(jnp.int32, table.shape, 1) < 64
    cosine = jnp.where(first, table, turned)
    sine = jnp.where(first, -turned, table)
    return u * cosine + pltpu.roll(u, 64, 1) * sine


def kernel(tok_in, table, qw, kw, vw, out,
           tok, rq, rk, rv, tq, csq, wkv, wq, kb, vb, qt, acc, top, proj, sbuf, osend, obuf,
           tok_s, loc_s, zs, zr, ws, wr, ts, tr, fs, fr,
           s_a, r_a, x_a, s_b, r_b, x_b, s_c, r_c, x_c, s_d, r_d, x_d, os_, or_, outs_):
    c, f = lax.axis_index("ctx"), lax.axis_index("fsdp")
    zl, x, y = c // 16, lax.rem(c // 4, 4), lax.rem(c, 4)
    zh, k = f // 2, lax.rem(f, 2)
    col = x * 4 + y
    at = {"zl": zl, "x": x, "y": y, "f": f}
    head = zl * 2 + k

    def device(zh_, zl_, k_):
        return {"ctx": zl_ * 16 + col, "fsdp": zh_ * 2 + k_}

    def remote(src, dst, ss, rs, dev):
        return pltpu.make_async_remote_copy(src_ref=src, dst_ref=dst, send_sem=ss, recv_sem=rs, device_id=dev,
                                            device_id_type=pl.DeviceIdType.MESH)

    core = device(zh, zl, 1 - k)
    chip = device(zh, 1 - zl, k)
    diagonal = device(zh, 1 - zl, 1 - k)
    step_a = 1 + 2 * zl
    slab_a = lax.rem(zh + 4 - step_a, 4)
    slab_c = lax.rem(zh + step_a, 4)
    slab_b = lax.rem(zh + 2, 4)
    push_to = [(step_a, slab_a, zl_, k_) for zl_ in (1 - zl, zl) for k_ in (0, 1)] + [(2, slab_b, 1 - zl, k_) for k_ in (0, 1)]

    barrier = pltpu.get_barrier_semaphore()
    ring = PlaneGather(at, None, (None, None, None), None, None)
    friends = [device(slab_b, 1 - zl, k_) for k_ in (0, 1)]
    friends += [device(slab_a, zl_, k_) for zl_ in (0, 1) for k_ in (0, 1)]
    friends += [device(slab_c, zl, k_) for k_ in (0, 1)]
    friends += [core, chip, diagonal]
    friends += [ring.neighbour(0, axis, step) for axis in (0, 1) for step in (1, 3)]
    for friend in friends:
        pl.semaphore_signal(barrier, inc=1, device_id=friend, device_id_type=pl.DeviceIdType.MESH)

    rows = pl.ds(pl.multiple_of(col * 32, 32), 32)
    loads = [pltpu.make_async_copy(tok_in.at[pl.ds(i * 64, 64), :], tok.at[pl.ds(i * 64, 64), :], tok_s.at[i]) for i in (0, 1)]
    staged = [pltpu.make_async_copy(src.at[rows, :], dst, tok_s.at[2 + i])
              for i, (src, dst) in enumerate(((kw, rk), (vw, rv), (qw, rq)))]
    own = [
        pltpu.make_async_copy(kw.at[:, pl.ds(pl.multiple_of(head * 128, 128), 128)], wkv.at[k, :, pl.ds(0, 128)], loc_s.at[0]),
        pltpu.make_async_copy(vw.at[:, pl.ds(pl.multiple_of(head * 128, 128), 128)], wkv.at[k, :, pl.ds(128, 128)], loc_s.at[1]),
        pltpu.make_async_copy(qw.at[:, pl.ds(pl.multiple_of(head * 512, 512), 512)], wq.at[k], loc_s.at[2]),
    ]
    for copy in loads + staged + own:
        copy.start()

    def norm_rows(i, _):
        line = pl.ds(pl.multiple_of(i * 16, 16), 16)
        values = tok[line, :].astype(F32)
        inverse = lax.rsqrt(jnp.mean(values * values, axis=-1, keepdims=True) + EPS)
        tq[k, line, :] = (values * inverse * table[:, 0:4096]).astype(BF16)
        return 0

    for copy in staged:
        copy.wait()

    pl.semaphore_wait(barrier, len(friends))

    def pushes(n, what):
        r, slab, zl_, k_ = push_to[n]
        j = zl_ * 2 + k_
        index = r * 2 + k
        dev = device(slab, zl_, k_)
        narrow = pl.ds(pl.multiple_of(j * 128, 128), 128)
        wide = pl.ds(pl.multiple_of(j * 512, 512), 512)
        src, dst = (
            (rk.at[:, narrow], wkv.at[index, rows, pl.ds(0, 128)]),
            (rv.at[:, narrow], wkv.at[index, rows, pl.ds(128, 128)]),
            (rq.at[:, wide], wq.at[index, rows, :]),
        )[what]
        if what == 2 and n < 2:
            src, dst = qw.at[:, wide], wq.at[index]
            return remote(src, dst, zs.at[2], zr.at[2], dev)
        return remote(src, dst, zs.at[what // 2], zr.at[what // 2], dev)

    def whole(ref, sem):
        pltpu.make_async_copy(ref, ref, sem).wait()

    for n in (4, 5, 0, 1, 2, 3):
        pushes(n, 0).start()
        pushes(n, 1).start()
    for n in (4, 5, 2, 3):
        pushes(n, 2).start()

    for i, copy in enumerate(loads):
        copy.wait()
        lax.fori_loop(i * 4, i * 4 + 4, norm_rows, 0)
    step_in = lax.broadcasted_iota(jnp.int32, (128, 128), 0)
    place = table[:, 4096:4224]
    column = jnp.where(step_in < 64, place[:, 0:1], place[:, 64:65]) + lax.rem(step_in, 64).astype(F32)
    angles = column * table[:, 4224:4352]
    first_half = lax.broadcasted_iota(jnp.int32, (128, 128), 1) < 64
    csq[k, 0:128, :] = jnp.where(first_half, jnp.cos(angles), jnp.sin(angles))
    csq[k, 128:136, :] = jnp.broadcast_to(place, (8, 128))

    other = zl * 2 + (1 - k)
    to_core = [
        remote(kw.at[:, pl.ds(pl.multiple_of(other * 128, 128), 128)], wkv.at[k, :, pl.ds(0, 128)], ws.at[0], wr.at[0], core),
        remote(vw.at[:, pl.ds(pl.multiple_of(other * 128, 128), 128)], wkv.at[k, :, pl.ds(128, 128)], ws.at[1], wr.at[1], core),
        remote(qw.at[:, pl.ds(pl.multiple_of(other * 512, 512), 512)], wq.at[k], ws.at[2], wr.at[2], core),
        remote(tq.at[k], tq.at[k], ws.at[3], wr.at[3], core),
        remote(csq.at[k], csq.at[k], ws.at[4], wr.at[4], core),
    ]
    for copy in to_core:
        copy.start()

    def quarter(q, i):
        return tq.at[q, :, pl.ds(i * 1024, 1024)]

    def to_chip(i):
        if i == 0:
            return remote(csq.at[k], csq.at[2 + k], ts.at[0], tr.at[0], chip)
        return remote(quarter(k, i - 1), quarter(2 + k, i - 1), ts.at[i], tr.at[i], chip)

    def from_chip(i):
        ref = csq.at[2 + k] if i == 0 else quarter(2 + k, i - 1)
        return remote(ref, ref, ts.at[i], tr.at[i], chip)

    def onward(i):
        ref = csq.at[2 + k] if i == 0 else quarter(2 + k, i - 1)
        return remote(ref, ref, fs.at[i], fr.at[i], core)

    def handed(i):
        ref = csq.at[3 - k] if i == 0 else quarter(3 - k, i - 1)
        return remote(ref, ref, fs.at[i], fr.at[i], core)

    for i in range(5):
        to_chip(i).start()

    def pass_on(*which):
        for i in which:
            from_chip(i).wait_recv()
            onward(i).start()

    def part(g, h, p):
        return wkv.at[pl.ds(2 + 3 * g, 3), pl.ds(pl.multiple_of(p * 32 + 16 * h, 16), 16), :]

    def part_q(g, h, p):
        return wq.at[pl.ds(2 + 2 * zl + 2 * g, 2), pl.ds(pl.multiple_of(p * 32 + 16 * h, 16), 16), :]

    wkv_g = PlaneGather(at, part, (s_a, r_a, x_a), lambda n, h: 0, (wkv.at[0:6, 0:480],))
    wq_g = PlaneGather(at, part_q, (s_b, r_b, x_b), lambda n, h: 0, (wq.at[0:4, 0:480],))
    kv_g = [PlaneGather(at, lambda g, h, p, m=m: vb.at[g, p, m] if h else kb.at[g, p, m], sems, lambda n, h: n * 2 + h,
                        (kb.at[:, 0:15, 0], vb.at[:, 0:15, 0]))
            for m, sems in enumerate(((s_c, r_c, x_c), (s_d, r_d, x_d)))]

    def kv_third(m, n):
        whole(kb.at[:, 0, 0], kv_g[m].rest(n, 0))
        whole(vb.at[:, 0, 0], kv_g[m].rest(n, 1))

    def kv_fourth(m):
        whole(kb.at[:, 0:4, 0], kv_g[m].rest(4, 0))
        whole(vb.at[:, 0:4, 0], kv_g[m].rest(4, 1))

    def both(step):
        for g in (0, 1):
            step(g)

    def each(step, lo, hi):
        def body(n, _):
            for g in (0, 1):
                step(g, n)
            return 0

        lax.fori_loop(lo, hi, body, 0)

    def third(gather, n):
        for g in (0, 1):
            gather.s3(g, n)

    def sideways(gather):
        for g in (0, 1):
            gather.second(g, 0, 0)

    def features(lo, count, r):
        start = pl.multiple_of(lax.rem(zh + r, 4) * 1024, 1024)
        return tq[lo:lo + count, :, pl.ds(start, 1024)].reshape(count * 128, 1024)

    lane = lax.broadcasted_iota(jnp.int32, (1, 128), 1)
    offset = lax.rem(lane, 64).astype(F32)

    def accumulate(r, lo, count, w, width):
        part = jnp.dot(features(lo, count, r), w, preferred_element_type=F32)
        size = count * 128

        @pl.when(r == 0)
        def _():
            proj[0:size, 0:width] = part

        @pl.when(r > 0)
        def _():
            proj[0:size, 0:width] = proj[0:size, 0:width] + part

    def make_kv(m):
        def project(r, _):
            accumulate(r, 2 * m, 2, wkv[pl.ds(2 * r, 2)].reshape(1024, 256), 256)
            return 0

        lax.fori_loop(0, 4, project, 0)
        for g in (0, 1):
            i = m * 2 + g
            key = rotate(proj[g * 128:g * 128 + 128, 0:128], csq[i, 0:128, :])
            kb[g, col, m, 0:128, :] = key.astype(BF16)
            vb[g, col, m] = proj[g * 128:g * 128 + 128, 128:256].T.astype(BF16)
            block = (csq[i, 128:129, :] - offset) * (1.0 / 64.0)
            kb[g, col, m, 128:144, :] = jnp.broadcast_to(block, (16, 128)).astype(BF16)

    def project_q(q, _):
        near = 3 - 2 * zl
        r = jnp.where(q == 0, 0, jnp.where(q == 1, near, jnp.where(q == 2, 2, 4 - near)))
        accumulate(r, 0, 4, wq[pl.ds(2 * r, 2)].reshape(1024, 512), 512)
        return 0

    whole(wkv.at[2:8, 0:32], zr.at[0])
    kv_a, kv_b = kv_g
    edge = lax.broadcasted_iota(jnp.int32, (128, 128), 0)
    for n in (0, 1):
        pushes(n, 2).start()
    both(wkv_g.first)
    sideways(wkv_g)
    acc[...] = jnp.zeros_like(acc)
    top[...] = jnp.full_like(top, FLOOR)
    both(wkv_g.relay)
    both(wkv_g.s1)
    whole(wq.at[2:6, 0:32], zr.at[1])
    both(wq_g.first)
    both(wkv_g.s2)
    third(wkv_g, 0)
    sideways(wq_g)
    third(wkv_g, 2)
    pass_on(0)
    third(wkv_g, 1)
    third(wkv_g, 3)
    both(wq_g.relay)
    both(wq_g.s1)
    pass_on(1)
    third(wq_g, 0)
    both(wq_g.s2)
    whole(wkv.at[0:6, 0:256], x_a.at[0])
    own[0].wait()
    own[1].wait()
    for i in (0, 1, 3, 4):
        to_core[i].wait_recv()
    make_kv(0)
    both(kv_a.first)
    sideways(kv_a)
    third(wq_g, 2)
    pass_on(2)
    third(wq_g, 3)
    third(wq_g, 1)
    both(kv_a.relay)
    pass_on(3, 4)
    both(kv_a.s1)
    for i in range(5):
        handed(i).wait_recv()
    make_kv(1)
    both(kv_b.first)
    both(kv_a.s2)
    sideways(kv_b)
    own[2].wait()
    to_core[2].wait_recv()
    for i in range(4):
        block = (csq[i, 128:129, :] - offset) * (1.0 / 64.0)
        later = jnp.where(edge.astype(F32) > block, FLOOR, 0.0).astype(BF16)
        for hd in range(GROUP):
            at_col = ((i // 2) * GROUP + hd) * 128
            qt[i % 2, 128:256, at_col:at_col + 128] = later
    lax.fori_loop(0, 1, project_q, 0)
    whole(wq.at[0:2], zr.at[2])
    lax.fori_loop(1, 2, project_q, 0)
    third(kv_a, 0)
    third(kv_a, 1)
    whole(wq.at[0:4, 0:256], x_b.at[0])
    lax.fori_loop(2, 4, project_q, 0)
    for i in range(4):
        for hd in range(GROUP):
            u = rotate(proj[pl.ds(i * 128, 128), pl.ds(hd * 128, 128)], csq[i, 0:128, :])
            at_col = ((i // 2) * GROUP + hd) * 128
            qt[i % 2, 0:128, at_col:at_col + 128] = u.T.astype(BF16)
    both(kv_b.relay)
    third(kv_a, 2)
    third(kv_a, 3)

    scale = HEAD ** -0.5 * LOG2E
    upper = edge < 64
    across = lax.broadcasted_iota(jnp.int32, (128, 128), 1)
    triangle = jnp.where((edge > across) & ((edge < 64) == (across < 64)), FLOOR, 0.0)
    numbers = across.astype(F32)
    ones = jnp.ones((16, 512), BF16)

    def attend(i, halves, groups=(0, 1)):
        m, turn = i // 4, lax.rem(i, 4)
        ends = (turn == 0) | (turn == 3)
        slots = []
        for e in range(4):
            da = around(jnp.where(ends, e, 2 * (turn - 1) + e // 2))
            db = jnp.where(turn == 0, 0, jnp.where(turn == 3, 2, 3 - 2 * (e % 2)))
            slots.append((da, db))
        work = []
        for g in groups:
            keys, values, runs = [], [], []
            for da, db in slots:
                p = kv_g[0].slot(g, da, db)
                keys.append(kb[g, p, m, 0:128, :])
                values.append(vb[g, p, m])
                block = kb[g, p, m, 128:144, :].astype(F32)[0:1, :]
                run = jnp.where(upper, block[:, 0:1], block[:, 64:65])
                runs.append(jnp.where(run == numbers, 1.0, 0.0).astype(BF16))
            keys = jnp.concatenate([jnp.concatenate(keys, axis=0), jnp.concatenate(runs, axis=0)], axis=1)
            values = jnp.concatenate([jnp.concatenate(values, axis=1), ones], axis=0)
            for half in halves:
                own_run = triangle * jnp.where((turn == 0) & (m == half), 1.0, 0.0)
                for tile in (0, 1):
                    work.append((g, keys, values, own_run, pl.ds(pl.multiple_of(half * 512 + tile * 256, 256), 256)))

        def score(t):
            g, keys, _, own_run, cols = work[t]
            scores = jnp.dot(keys, qt[g, :, cols], preferred_element_type=F32)
            first = scores[0:128] + jnp.concatenate([own_run, own_run], axis=1)
            sbuf[t % 2, 0:128] = first
            sbuf[t % 2, 128:512] = scores[128:512]
            return jnp.maximum(jnp.max(first, axis=0, keepdims=True), jnp.max(scores[128:512], axis=0, keepdims=True))

        best = score(0)
        for t in range(len(work)):
            g, _, values, _, cols = work[t]
            following = score(t + 1) if t + 1 < len(work) else None
            before = top[g, 0:1, cols]
            now = jnp.maximum(before, best)
            probs = jnp.exp2((sbuf[t % 2] - now) * scale).astype(BF16)
            factor = jnp.exp2((before - now) * scale)
            acc[g, :, cols] = acc[g, :, cols] * factor + jnp.dot(values, probs, preferred_element_type=F32)
            top[g, 0:1, cols] = now
            best = following

    def settle(m, g):
        for hd in range(GROUP):
            at_col = m * 512 + hd * 128
            one = acc[g, 0:128, at_col:at_col + 128] / acc[g, 128:129, at_col:at_col + 128]
            osend[m * 2 + g, :, hd * 128:hd * 128 + 128] = one.T.astype(BF16)

    def give_far(g):
        n = lax.rem(g + k, 2)
        return remote(osend.at[2 + g], obuf.at[head], os_.at[n], or_.at[n], device(zh, 1 - zl, g))

    def give_near():
        return remote(osend.at[1 - k], obuf.at[head], os_.at[2], or_.at[2], core)

    def take(n):
        j = ((1 - zl) * 2 + k, (1 - zl) * 2 + 1 - k, zl * 2 + 1 - k)[n]
        return j, remote(obuf.at[j], obuf.at[j], os_.at[n], or_.at[n], core)

    def round_both(i, _):
        @pl.when(i == 1)
        def _():
            both(kv_b.s1)
            kv_third(0, 0)
            kv_third(0, 1)

        @pl.when(i == 2)
        def _():
            both(kv_b.s2)
            kv_third(0, 2)
            kv_third(0, 3)

        @pl.when(i == 3)
        def _():
            third(kv_b, 1)
            third(kv_b, 0)
            kv_fourth(0)

        attend(i, (1, 0))
        return 0

    def round_one(step, _):
        @pl.when(step == 0)
        def _():
            third(kv_b, 2)
            third(kv_b, 3)

        @pl.when(step == 1)
        def _():
            kv_third(1, 0)
            kv_third(1, 1)

        @pl.when(step == 2)
        def _():
            kv_third(1, 2)
            kv_third(1, 3)

        attend(4 + step, (1,))
        return 0

    def last_round(g, _):
        attend(7, (1,), (g,))
        settle(1, g)
        give_far(g).start()
        return 0

    def own_round(i, _):
        attend(i, (0,))
        return 0

    lax.fori_loop(0, 4, round_both, 0)
    lax.fori_loop(0, 3, round_one, 0)
    kv_fourth(1)
    lax.fori_loop(0, 2, last_round, 0)
    lax.fori_loop(4, 8, own_round, 0)
    settle(0, 0)
    settle(0, 1)
    give_near().start()

    def store(src, j, n):
        return pltpu.make_async_copy(src, out.at[:, pl.ds(pl.multiple_of(j * 512, 512), 512)], outs_.at[n])

    last = [store(osend.at[k], head, 3)]
    last[0].start()
    whole(wkv.at[2:8, 0:32], zs.at[0])
    whole(wq.at[2:6, 0:32], zs.at[1])
    whole(wq.at[0:2], zs.at[2])
    for copy in to_core:
        copy.wait_send()
    for i in range(5):
        to_chip(i).wait_send()
        onward(i).wait_send()
    for gather in (wkv_g, wq_g, kv_g[0], kv_g[1]):
        gather.finish()
    for n in (2, 0, 1):
        j, arrival = take(n)
        arrival.wait_recv()
        last.append(store(obuf.at[j], j, n))
        last[-1].start()
    give_far(0).wait_send()
    give_far(1).wait_send()
    give_near().wait_send()
    for copy in last:
        copy.wait()


def on_device(tokens, positions, norm_gain, query_weight, key_weight, value_matrix):
    frequency = BASE ** (-(jnp.arange(HEAD // 2, dtype=F32) * 2.0) / HEAD)
    table = jnp.concatenate([norm_gain, positions[0].astype(F32), frequency, frequency])[None, :]
    vmem = pl.BlockSpec(memory_space=pltpu.VMEM)
    anywhere = pl.BlockSpec(memory_space=pl.ANY)
    far = pl.BlockSpec(memory_space=pltpu.HBM)
    dma = pltpu.SemaphoreType.DMA
    result = pl.pallas_call(
        kernel,
        out_shape=jax.ShapeDtypeStruct((128, 2048), BF16),
        in_specs=[far, vmem, far, far, far],
        out_specs=anywhere,
        scratch_shapes=[
            pltpu.VMEM((128, 4096), BF16),
            pltpu.VMEM((32, 2048), BF16),
            pltpu.VMEM((32, 512), BF16),
            pltpu.VMEM((32, 512), BF16),
            pltpu.VMEM((4, 128, 4096), BF16),
            pltpu.VMEM((4, 136, 128), F32),
            pltpu.VMEM((8, 512, 256), BF16),
            pltpu.VMEM((8, 512, 512), BF16),
            pltpu.VMEM((2, 16, 2, 144, 128), BF16),
            pltpu.VMEM((2, 16, 2, 128, 128), BF16),
            pltpu.VMEM((2, 256, 1024), BF16),
            pltpu.VMEM((2, 144, 1024), F32),
            pltpu.VMEM((2, 8, 1024), F32),
            pltpu.VMEM((512, 512), F32),
            pltpu.VMEM((2, 512, 256), F32),
            pltpu.VMEM((4, 128, 512), BF16),
            pltpu.VMEM((4, 128, 512), BF16),
            dma((5,)), dma((3,)), dma((3,)), dma((3,)), dma((5,)), dma((5,)), dma((5,)), dma((5,)), dma((5,)), dma((5,)),
            dma((1,)), dma((2, 14)), dma((1,)), dma((1,)), dma((2, 14)), dma((1,)),
            dma((2,)), dma((2, 14)), dma((10,)), dma((2,)), dma((2, 14)), dma((10,)),
            dma((3,)), dma((3,)), dma((4,)),
        ],
        compiler_params=pltpu.CompilerParams(
            collective_id=0, has_side_effects=True, vmem_limit_bytes=53 * 1024 * 1024),
    )(tokens[0], table, query_weight, key_weight, value_matrix)
    return result[None]


def solution(mesh):
    placed = (
        P("fsdp", "ctx", None),
        P("fsdp", "ctx"),
        P(),
        P("fsdp", None),
        P("fsdp", None),
        P("fsdp", None),
    )
    return jax.shard_map(
        on_device, mesh=mesh, in_specs=placed, out_specs=P("fsdp", "ctx", None), check_vma=False
    )
```

```python
import math

import jax
import jax.numpy as jnp
from jax import lax
from jax.experimental import pallas as pl
from jax.experimental.pallas import tpu as pltpu
from jax.sharding import PartitionSpec as P

HEAD = 128
GROUP = 4
EPS = 1e-05
BASE = 500000.0
FLOOR = -1e30
LOG2E = math.log2(math.e)
F32, BF16 = jnp.float32, jnp.bfloat16


def around(n):
    return jnp.where(n == 0, 0, jnp.where(n == 1, 3, jnp.where(n == 2, 1, 2)))


class PlaneGather:
    def __init__(self, at, piece, sems, shared, sent):
        self.at, self.piece, self.sent = at, piece, sent
        self.send_sem, self.recv_sem, self.rest_sem, self.shared = *sems, shared

    def slot(self, g, da, db):
        if isinstance(g, int):
            dx, dy = (da, db) if g == 0 else (db, da)
        else:
            dx, dy = jnp.where(g == 0, da, db), jnp.where(g == 0, db, da)
        return lax.rem(self.at["x"] + dx, 4) * 4 + lax.rem(self.at["y"] + dy, 4)

    def neighbour(self, g, axis, step):
        along_x = (axis == 0) == (g == 0)
        dx, dy = (step, 0) if along_x else (0, step)
        ctx = self.at["zl"] * 16 + lax.rem(self.at["x"] + dx, 4) * 4 + lax.rem(self.at["y"] + dy, 4)
        return {"ctx": ctx, "fsdp": self.at["f"]}

    def early(self, g, d, h):
        return self.recv_sem.at[g, (0, 2, 4, 0)[d] + h] if d != 1 else self.recv_sem.at[g, 2 + h]

    def relayed(self, g, n, h):
        return self.recv_sem.at[g, 6 + n * 2 + h]

    def rest(self, n, h):
        return self.rest_sem.at[self.shared(n, h)]

    def copy(self, g, h, p, recv_sem, device):
        ref = self.piece(g, h, p)
        return pltpu.make_async_remote_copy(
            src_ref=ref, dst_ref=ref, send_sem=self.send_sem.at[min(h, self.send_sem.shape[0] - 1)], recv_sem=recv_sem,
            device_id=device, device_id_type=pl.DeviceIdType.MESH)

    def send(self, g, h, p, recv_sem, axis, step):
        self.copy(g, h, p, recv_sem, self.neighbour(g, axis, step)).start()

    def arrived(self, g, h, p, recv_sem):
        self.copy(g, h, p, recv_sem, self.neighbour(g, 0, 1)).wait_recv()

    def first(self, g):
        p = self.slot(g, 0, 0)
        for h in (0, 1):
            self.send(g, h, p, self.early(g, 3, h), 0, 1)
            self.send(g, h, p, self.early(g, 1, h), 0, 3)

    def second(self, g, n, da):
        p = self.slot(g, da, 0)
        for h in (0, 1):
            self.send(g, h, p, self.rest(n, h) if h else self.relayed(g, n, 0), 1, 1)
            self.send(g, h, p, self.relayed(g, n, 1) if h else self.rest(n, h), 1, 3)

    def relay(self, g):
        for d, h, step in ((3, 0, 1), (1, 1, 3)):
            p = self.slot(g, d, 0)
            self.arrived(g, h, p, self.early(g, d, h))
            self.send(g, h, p, self.early(g, 2, h), 0, step)

    def s1(self, g):
        for n, d, h in ((1, 3, 1), (2, 1, 0)):
            self.arrived(g, h, self.slot(g, d, 0), self.early(g, d, h))
            self.second(g, n, d)

    def s2(self, g):
        p = self.slot(g, 2, 0)
        for h in (0, 1):
            self.arrived(g, h, p, self.early(g, 2, h))
        self.second(g, 3, 2)

    def s3(self, g, n):
        d = around(n)
        for db, h, step in ((3, 0, 1), (1, 1, 3)):
            p = self.slot(g, d, db)
            self.arrived(g, h, p, self.relayed(g, n, h))
            self.send(g, h, p, self.rest(4, h), 1, step)

    def gathered(self, ref, sem):
        pltpu.make_async_copy(ref, ref, sem).wait()

    def finish(self):
        for h, ref in enumerate(self.sent):
            self.gathered(ref, self.send_sem.at[h])


def rotate(u, table):
    turned = pltpu.roll(table, 64, 1)
    first = lax.broadcasted_iota(jnp.int32, table.shape, 1) < 64
    cosine = jnp.where(first, table, turned)
    sine = jnp.where(first, -turned, table)
    return u * cosine + pltpu.roll(u, 64, 1) * sine


def kernel(tok_in, table, qw, kw, vw, out,
           tok, gain, rq, rk, rv, tq, csq, wkv, wq, kb, vb, qt, acc, top, proj, sbuf, osend, obuf,
           tok_s, loc_s, zs, zr, ws, wr, ts, tr, fs, fr,
           s_a, r_a, x_a, s_b, r_b, x_b, s_c, r_c, x_c, s_d, r_d, x_d, os_, or_, outs_):
    c, f = lax.axis_index("ctx"), lax.axis_index("fsdp")
    zl, x, y = c // 16, lax.rem(c // 4, 4), lax.rem(c, 4)
    zh, k = f // 2, lax.rem(f, 2)
    col = x * 4 + y
    at = {"zl": zl, "x": x, "y": y, "f": f}
    head = zl * 2 + k

    def device(zh_, zl_, k_):
        return {"ctx": zl_ * 16 + col, "fsdp": zh_ * 2 + k_}

    def remote(src, dst, ss, rs, dev):
        return pltpu.make_async_remote_copy(src_ref=src, dst_ref=dst, send_sem=ss, recv_sem=rs, device_id=dev,
                                            device_id_type=pl.DeviceIdType.MESH)

    core = device(zh, zl, 1 - k)
    chip = device(zh, 1 - zl, k)
    diagonal = device(zh, 1 - zl, 1 - k)
    step_a = 1 + 2 * zl
    slab_a = lax.rem(zh + 4 - step_a, 4)
    slab_c = lax.rem(zh + step_a, 4)
    slab_b = lax.rem(zh + 2, 4)
    push_to = [(step_a, slab_a, zl_, k_) for zl_ in (1 - zl, zl) for k_ in (0, 1)] + [(2, slab_b, 1 - zl, k_) for k_ in (0, 1)]

    barrier = pltpu.get_barrier_semaphore()
    ring = PlaneGather(at, None, (None, None, None), None, None)
    friends = [device(slab_b, 1 - zl, k_) for k_ in (0, 1)]
    friends += [device(slab_a, zl_, k_) for zl_ in (0, 1) for k_ in (0, 1)]
    friends += [device(slab_c, zl, k_) for k_ in (0, 1)]
    friends += [core, chip, diagonal]
    friends += [ring.neighbour(0, axis, step) for axis in (0, 1) for step in (1, 3)]
    for friend in friends:
        pl.semaphore_signal(barrier, inc=1, device_id=friend, device_id_type=pl.DeviceIdType.MESH)

    rows = pl.ds(pl.multiple_of(col * 32, 32), 32)
    loads = [pltpu.make_async_copy(tok_in.at[pl.ds(i * 64, 64), :], tok.at[pl.ds(i * 64, 64), :], tok_s.at[i]) for i in (0, 1)]
    staged = [pltpu.make_async_copy(src.at[rows, :], dst, tok_s.at[2 + i])
              for i, (src, dst) in enumerate(((kw, rk), (vw, rv), (qw, rq)))]
    own = [
        pltpu.make_async_copy(kw.at[:, pl.ds(pl.multiple_of(head * 128, 128), 128)], wkv.at[k, :, pl.ds(0, 128)], loc_s.at[0]),
        pltpu.make_async_copy(vw.at[:, pl.ds(pl.multiple_of(head * 128, 128), 128)], wkv.at[k, :, pl.ds(128, 128)], loc_s.at[1]),
        pltpu.make_async_copy(qw.at[:, pl.ds(pl.multiple_of(head * 512, 512), 512)], wq.at[k], loc_s.at[2]),
    ]
    for copy in loads + staged + own:
        copy.start()

    def norm_rows(i, _):
        line = pl.ds(pl.multiple_of(i * 16, 16), 16)
        values = tok[line, :].astype(F32)
        inverse = lax.rsqrt(jnp.mean(values * values, axis=-1, keepdims=True) + EPS)
        tq[k, line, :] = (values * inverse * gain[...]).astype(BF16)
        return 0

    for i in range(32):
        gain[:, i * 128:i * 128 + 128] = table[i:i + 1, :]
    for copy in staged:
        copy.wait()

    pl.semaphore_wait(barrier, len(friends))

    def pushes(n, what):
        r, slab, zl_, k_ = push_to[n]
        j = zl_ * 2 + k_
        index = r * 2 + k
        dev = device(slab, zl_, k_)
        narrow = pl.ds(pl.multiple_of(j * 128, 128), 128)
        wide = pl.ds(pl.multiple_of(j * 512, 512), 512)
        src, dst = (
            (rk.at[:, narrow], wkv.at[index, rows, pl.ds(0, 128)]),
            (rv.at[:, narrow], wkv.at[index, rows, pl.ds(128, 128)]),
            (rq.at[:, wide], wq.at[index, rows, :]),
        )[what]
        if what == 2 and n < 2:
            src, dst = qw.at[:, wide], wq.at[index]
            return remote(src, dst, zs.at[2], zr.at[2], dev)
        return remote(src, dst, zs.at[what // 2], zr.at[what // 2], dev)

    def whole(ref, sem):
        pltpu.make_async_copy(ref, ref, sem).wait()

    for n in (4, 5, 0, 1, 2, 3):
        pushes(n, 0).start()
        pushes(n, 1).start()
    for n in (4, 5, 2, 3):
        pushes(n, 2).start()

    for i, copy in enumerate(loads):
        copy.wait()
        lax.fori_loop(i * 4, i * 4 + 4, norm_rows, 0)
    step_in = lax.broadcasted_iota(jnp.int32, (128, 128), 0)
    place = table[32:33, :]
    column = jnp.where(step_in < 64, place[:, 0:1], place[:, 64:65]) + lax.rem(step_in, 64).astype(F32)
    angles = column * table[33:34, :]
    first_half = lax.broadcasted_iota(jnp.int32, (128, 128), 1) < 64
    csq[k, 0:128, :] = jnp.where(first_half, jnp.cos(angles), jnp.sin(angles))
    csq[k, 128:136, :] = jnp.broadcast_to(place, (8, 128))

    other = zl * 2 + (1 - k)
    to_core = [
        remote(kw.at[:, pl.ds(pl.multiple_of(other * 128, 128), 128)], wkv.at[k, :, pl.ds(0, 128)], ws.at[0], wr.at[0], core),
        remote(vw.at[:, pl.ds(pl.multiple_of(other * 128, 128), 128)], wkv.at[k, :, pl.ds(128, 128)], ws.at[1], wr.at[1], core),
        remote(qw.at[:, pl.ds(pl.multiple_of(other * 512, 512), 512)], wq.at[k], ws.at[2], wr.at[2], core),
        remote(tq.at[k], tq.at[k], ws.at[3], wr.at[3], core),
        remote(csq.at[k], csq.at[k], ws.at[4], wr.at[4], core),
    ]
    for copy in to_core:
        copy.start()

    def quarter(q, i):
        return tq.at[q, :, pl.ds(i * 1024, 1024)]

    def to_chip(i):
        if i == 0:
            return remote(csq.at[k], csq.at[2 + k], ts.at[0], tr.at[0], chip)
        return remote(quarter(k, i - 1), quarter(2 + k, i - 1), ts.at[i], tr.at[i], chip)

    def from_chip(i):
        ref = csq.at[2 + k] if i == 0 else quarter(2 + k, i - 1)
        return remote(ref, ref, ts.at[i], tr.at[i], chip)

    def onward(i):
        ref = csq.at[2 + k] if i == 0 else quarter(2 + k, i - 1)
        return remote(ref, ref, fs.at[i], fr.at[i], core)

    def handed(i):
        ref = csq.at[3 - k] if i == 0 else quarter(3 - k, i - 1)
        return remote(ref, ref, fs.at[i], fr.at[i], core)

    for i in range(5):
        to_chip(i).start()

    def pass_on(*which):
        for i in which:
            from_chip(i).wait_recv()
            onward(i).start()

    def part(g, h, p):
        return wkv.at[pl.ds(2 + 3 * g, 3), pl.ds(pl.multiple_of(p * 32 + 16 * h, 16), 16), :]

    def part_q(g, h, p):
        return wq.at[pl.ds(2 + 2 * zl + 2 * g, 2), pl.ds(pl.multiple_of(p * 32 + 16 * h, 16), 16), :]

    wkv_g = PlaneGather(at, part, (s_a, r_a, x_a), lambda n, h: 0, (wkv.at[0:6, 0:480],))
    wq_g = PlaneGather(at, part_q, (s_b, r_b, x_b), lambda n, h: 0, (wq.at[0:4, 0:480],))
    kv_g = [PlaneGather(at, lambda g, h, p, m=m: vb.at[g, p, m] if h else kb.at[g, p, m], sems, lambda n, h: n * 2 + h,
                        (kb.at[:, 0:15, 0], vb.at[:, 0:15, 0]))
            for m, sems in enumerate(((s_c, r_c, x_c), (s_d, r_d, x_d)))]

    def kv_third(m, n):
        whole(kb.at[:, 0, 0], kv_g[m].rest(n, 0))
        whole(vb.at[:, 0, 0], kv_g[m].rest(n, 1))

    def kv_fourth(m):
        whole(kb.at[:, 0:4, 0], kv_g[m].rest(4, 0))
        whole(vb.at[:, 0:4, 0], kv_g[m].rest(4, 1))

    def both(step):
        for g in (0, 1):
            step(g)

    def each(step, lo, hi):
        def body(n, _):
            for g in (0, 1):
                step(g, n)
            return 0

        lax.fori_loop(lo, hi, body, 0)

    def third(gather, n):
        for g in (0, 1):
            gather.s3(g, n)

    def sideways(gather):
        for g in (0, 1):
            gather.second(g, 0, 0)

    def features(lo, count, r):
        start = pl.multiple_of(lax.rem(zh + r, 4) * 1024, 1024)
        return tq[lo:lo + count, :, pl.ds(start, 1024)].reshape(count * 128, 1024)

    lane = lax.broadcasted_iota(jnp.int32, (1, 128), 1)
    offset = lax.rem(lane, 64).astype(F32)

    def accumulate(r, lo, count, w, width):
        part = jnp.dot(features(lo, count, r), w, preferred_element_type=F32)
        size = count * 128

        @pl.when(r == 0)
        def _():
            proj[0:size, 0:width] = part

        @pl.when(r > 0)
        def _():
            proj[0:size, 0:width] = proj[0:size, 0:width] + part

    def make_kv(m):
        def project(r, _):
            accumulate(r, 2 * m, 2, wkv[pl.ds(2 * r, 2)].reshape(1024, 256), 256)
            return 0

        lax.fori_loop(0, 4, project, 0)
        for g in (0, 1):
            i = m * 2 + g
            key = rotate(proj[g * 128:g * 128 + 128, 0:128], csq[i, 0:128, :])
            kb[g, col, m, 0:128, :] = key.astype(BF16)
            vb[g, col, m] = proj[g * 128:g * 128 + 128, 128:256].T.astype(BF16)
            block = (csq[i, 128:129, :] - offset) * (1.0 / 64.0)
            kb[g, col, m, 128:144, :] = jnp.broadcast_to(block, (16, 128)).astype(BF16)

    def project_q(q, _):
        near = 3 - 2 * zl
        r = jnp.where(q == 0, 0, jnp.where(q == 1, near, jnp.where(q == 2, 2, 4 - near)))
        accumulate(r, 0, 4, wq[pl.ds(2 * r, 2)].reshape(1024, 512), 512)
        return 0

    whole(wkv.at[2:8, 0:32], zr.at[0])
    kv_a, kv_b = kv_g
    edge = lax.broadcasted_iota(jnp.int32, (128, 128), 0)
    for n in (0, 1):
        pushes(n, 2).start()
    both(wkv_g.first)
    sideways(wkv_g)
    acc[...] = jnp.zeros_like(acc)
    top[...] = jnp.full_like(top, FLOOR)
    both(wkv_g.relay)
    both(wkv_g.s1)
    whole(wq.at[2:6, 0:32], zr.at[1])
    both(wq_g.first)
    both(wkv_g.s2)
    third(wkv_g, 0)
    sideways(wq_g)
    third(wkv_g, 2)
    pass_on(0)
    third(wkv_g, 1)
    third(wkv_g, 3)
    both(wq_g.relay)
    both(wq_g.s1)
    pass_on(1)
    third(wq_g, 0)
    both(wq_g.s2)
    whole(wkv.at[0:6, 0:256], x_a.at[0])
    own[0].wait()
    own[1].wait()
    for i in (0, 1, 3, 4):
        to_core[i].wait_recv()
    make_kv(0)
    both(kv_a.first)
    sideways(kv_a)
    third(wq_g, 2)
    pass_on(2)
    third(wq_g, 3)
    third(wq_g, 1)
    both(kv_a.relay)
    pass_on(3, 4)
    both(kv_a.s1)
    for i in range(5):
        handed(i).wait_recv()
    make_kv(1)
    both(kv_b.first)
    both(kv_a.s2)
    sideways(kv_b)
    own[2].wait()
    to_core[2].wait_recv()
    for i in range(4):
        block = (csq[i, 128:129, :] - offset) * (1.0 / 64.0)
        later = jnp.where(edge.astype(F32) > block, FLOOR, 0.0).astype(BF16)
        for hd in range(GROUP):
            at_col = ((i // 2) * GROUP + hd) * 128
            qt[i % 2, 128:256, at_col:at_col + 128] = later
    lax.fori_loop(0, 1, project_q, 0)
    whole(wq.at[0:2], zr.at[2])
    lax.fori_loop(1, 2, project_q, 0)
    third(kv_a, 0)
    third(kv_a, 1)
    whole(wq.at[0:4, 0:256], x_b.at[0])
    lax.fori_loop(2, 4, project_q, 0)
    for i in range(4):
        for hd in range(GROUP):
            u = rotate(proj[pl.ds(i * 128, 128), pl.ds(hd * 128, 128)], csq[i, 0:128, :])
            at_col = ((i // 2) * GROUP + hd) * 128
            qt[i % 2, 0:128, at_col:at_col + 128] = u.T.astype(BF16)
    both(kv_b.relay)
    third(kv_a, 2)
    third(kv_a, 3)

    scale = HEAD ** -0.5 * LOG2E
    upper = edge < 64
    across = lax.broadcasted_iota(jnp.int32, (128, 128), 1)
    triangle = jnp.where((edge > across) & ((edge < 64) == (across < 64)), FLOOR, 0.0)
    numbers = across.astype(F32)
    ones = jnp.ones((16, 512), BF16)

    def attend(i, halves, groups=(0, 1)):
        m, turn = i // 4, lax.rem(i, 4)
        ends = (turn == 0) | (turn == 3)
        slots = []
        for e in range(4):
            da = around(jnp.where(ends, e, 2 * (turn - 1) + e // 2))
            db = jnp.where(turn == 0, 0, jnp.where(turn == 3, 2, 3 - 2 * (e % 2)))
            slots.append((da, db))
        work = []
        for g in groups:
            keys, values, runs = [], [], []
            for da, db in slots:
                p = kv_g[0].slot(g, da, db)
                keys.append(kb[g, p, m, 0:128, :])
                values.append(vb[g, p, m])
                block = kb[g, p, m, 128:144, :].astype(F32)[0:1, :]
                run = jnp.where(upper, block[:, 0:1], block[:, 64:65])
                runs.append(jnp.where(run == numbers, 1.0, 0.0).astype(BF16))
            keys = jnp.concatenate([jnp.concatenate(keys, axis=0), jnp.concatenate(runs, axis=0)], axis=1)
            values = jnp.concatenate([jnp.concatenate(values, axis=1), ones], axis=0)
            for half in halves:
                own_run = triangle * jnp.where((turn == 0) & (m == half), 1.0, 0.0)
                for tile in (0, 1):
                    work.append((g, keys, values, own_run, pl.ds(pl.multiple_of(half * 512 + tile * 256, 256), 256)))

        def score(t):
            g, keys, _, own_run, cols = work[t]
            scores = jnp.dot(keys, qt[g, :, cols], preferred_element_type=F32)
            first = scores[0:128] + jnp.concatenate([own_run, own_run], axis=1)
            sbuf[t % 2, 0:128] = first
            sbuf[t % 2, 128:512] = scores[128:512]
            return jnp.maximum(jnp.max(first, axis=0, keepdims=True), jnp.max(scores[128:512], axis=0, keepdims=True))

        best = score(0)
        for t in range(len(work)):
            g, _, values, _, cols = work[t]
            following = score(t + 1) if t + 1 < len(work) else None
            before = top[g, 0:1, cols]
            now = jnp.maximum(before, best)
            probs = jnp.exp2((sbuf[t % 2] - now) * scale).astype(BF16)
            factor = jnp.exp2((before - now) * scale)
            acc[g, :, cols] = acc[g, :, cols] * factor + jnp.dot(values, probs, preferred_element_type=F32)
            top[g, 0:1, cols] = now
            best = following

    def settle(m, g):
        for hd in range(GROUP):
            at_col = m * 512 + hd * 128
            one = acc[g, 0:128, at_col:at_col + 128] / acc[g, 128:129, at_col:at_col + 128]
            osend[m * 2 + g, :, hd * 128:hd * 128 + 128] = one.T.astype(BF16)

    def give_far(g):
        n = lax.rem(g + k, 2)
        return remote(osend.at[2 + g], obuf.at[head], os_.at[n], or_.at[n], device(zh, 1 - zl, g))

    def give_near():
        return remote(osend.at[1 - k], obuf.at[head], os_.at[2], or_.at[2], core)

    def take(n):
        j = ((1 - zl) * 2 + k, (1 - zl) * 2 + 1 - k, zl * 2 + 1 - k)[n]
        return j, remote(obuf.at[j], obuf.at[j], os_.at[n], or_.at[n], core)

    def round_both(i, _):
        @pl.when(i == 1)
        def _():
            both(kv_b.s1)
            kv_third(0, 0)
            kv_third(0, 1)

        @pl.when(i == 2)
        def _():
            both(kv_b.s2)
            kv_third(0, 2)
            kv_third(0, 3)

        @pl.when(i == 3)
        def _():
            third(kv_b, 1)
            third(kv_b, 0)
            kv_fourth(0)

        attend(i, (1, 0))
        return 0

    def round_one(step, _):
        @pl.when(step == 0)
        def _():
            third(kv_b, 2)
            third(kv_b, 3)

        @pl.when(step == 1)
        def _():
            kv_third(1, 0)
            kv_third(1, 1)

        @pl.when(step == 2)
        def _():
            kv_third(1, 2)
            kv_third(1, 3)

        attend(4 + step, (1,))
        return 0

    def last_round(g, _):
        attend(7, (1,), (g,))
        settle(1, g)
        give_far(g).start()
        return 0

    def own_round(i, _):
        attend(i, (0,))
        return 0

    lax.fori_loop(0, 4, round_both, 0)
    lax.fori_loop(0, 3, round_one, 0)
    kv_fourth(1)
    lax.fori_loop(0, 2, last_round, 0)
    lax.fori_loop(4, 8, own_round, 0)
    settle(0, 0)
    settle(0, 1)
    give_near().start()

    def store(src, j, n):
        return pltpu.make_async_copy(src, out.at[:, pl.ds(pl.multiple_of(j * 512, 512), 512)], outs_.at[n])

    last = [store(osend.at[k], head, 3)]
    last[0].start()
    whole(wkv.at[2:8, 0:32], zs.at[0])
    whole(wq.at[2:6, 0:32], zs.at[1])
    whole(wq.at[0:2], zs.at[2])
    for copy in to_core:
        copy.wait_send()
    for i in range(5):
        to_chip(i).wait_send()
        onward(i).wait_send()
    for gather in (wkv_g, wq_g, kv_g[0], kv_g[1]):
        gather.finish()
    for n in (2, 0, 1):
        j, arrival = take(n)
        arrival.wait_recv()
        last.append(store(obuf.at[j], j, n))
        last[-1].start()
    give_far(0).wait_send()
    give_far(1).wait_send()
    give_near().wait_send()
    for copy in last:
        copy.wait()


def on_device(tokens, positions, norm_gain, query_weight, key_weight, value_matrix):
    frequency = BASE ** (-(jnp.arange(HEAD // 2, dtype=F32) * 2.0) / HEAD)
    lines = [norm_gain.reshape(32, HEAD), positions.astype(F32), jnp.concatenate([frequency, frequency])[None, :]]
    table = jnp.concatenate(lines, axis=0)
    vmem = pl.BlockSpec(memory_space=pltpu.VMEM)
    anywhere = pl.BlockSpec(memory_space=pl.ANY)
    far = pl.BlockSpec(memory_space=pltpu.HBM)
    dma = pltpu.SemaphoreType.DMA
    result = pl.pallas_call(
        kernel,
        out_shape=jax.ShapeDtypeStruct((128, 2048), BF16),
        in_specs=[far, vmem, far, far, far],
        out_specs=anywhere,
        scratch_shapes=[
            pltpu.VMEM((128, 4096), BF16),
            pltpu.VMEM((1, 4096), F32),
            pltpu.VMEM((32, 2048), BF16),
            pltpu.VMEM((32, 512), BF16),
            pltpu.VMEM((32, 512), BF16),
            pltpu.VMEM((4, 128, 4096), BF16),
            pltpu.VMEM((4, 136, 128), F32),
            pltpu.VMEM((8, 512, 256), BF16),
            pltpu.VMEM((8, 512, 512), BF16),
            pltpu.VMEM((2, 16, 2, 144, 128), BF16),
            pltpu.VMEM((2, 16, 2, 128, 128), BF16),
            pltpu.VMEM((2, 256, 1024), BF16),
            pltpu.VMEM((2, 144, 1024), F32),
            pltpu.VMEM((2, 8, 1024), F32),
            pltpu.VMEM((512, 512), F32),
            pltpu.VMEM((2, 512, 256), F32),
            pltpu.VMEM((4, 128, 512), BF16),
            pltpu.VMEM((4, 128, 512), BF16),
            dma((5,)), dma((3,)), dma((3,)), dma((3,)), dma((5,)), dma((5,)), dma((5,)), dma((5,)), dma((5,)), dma((5,)),
            dma((1,)), dma((2, 14)), dma((1,)), dma((1,)), dma((2, 14)), dma((1,)),
            dma((2,)), dma((2, 14)), dma((10,)), dma((2,)), dma((2, 14)), dma((10,)),
            dma((3,)), dma((3,)), dma((4,)),
        ],
        compiler_params=pltpu.CompilerParams(
            collective_id=0, has_side_effects=True, vmem_limit_bytes=53 * 1024 * 1024),
    )(tokens[0], table, query_weight, key_weight, value_matrix)
    return result[None]


def solution(mesh):
    placed = (
        P("fsdp", "ctx", None),
        P("fsdp", "ctx"),
        P(),
        P("fsdp", None),
        P("fsdp", None),
        P("fsdp", None),
    )
    return jax.shard_map(
        on_device, mesh=mesh, in_specs=placed, out_specs=P("fsdp", "ctx", None), check_vma=False
    )
```
